32 devices in a mesh: seq: 2 (over y), section: 4 (over x, core), tp: 4 (over z).
Axes of the slice: x: 2, y: 2, z: 4, core: 2. Of those that a mesh axis runs over, the one named last changes fastest.
Arguments:
- token_ids: int32 [128], P('seq'), may hold values from 0 to 65535
- embed_columns: bfloat16 [4096, 65536], P(('tp', 'seq')), may hold values from -6 to 6
- norm_gain: bfloat16 [4, 4096], P('section'), may hold values from 0.099609375 to 1.8984375
- qkv_weight: bfloat16 [4, 4096, 4096], P('section', 'seq', 'tp'), may hold values from -1 to 1
- out_weight: bfloat16 [4, 4096, 2048], P('section', 'seq', 'tp'), may hold values from -0.125 to 0.125
Outputs:
- layer_states: bfloat16 [4, 128, 4096], P('section', 'seq', 'tp')
The draws below stay inside these ranges and needn't reach their ends.
All inputs are finite; a program needn't handle non-finite values.
Results may differ from the reference program's by a relative error of at most 0.02.
Values may be sent and summed in bfloat16 or wider, within the bound.
No kernel may reach another device: no remote copies, remote signals or barrier semaphores. Data moves between devices by JAX's collectives and lax.ppermute only.
A program may use at most 192 MiB of HBM per device.

```python
import math
import jax
import jax.numpy as jnp
import numpy as np
from jax import lax

D = 4096
QUERY_HEADS = 16
KEY_VALUE_HEADS = 8
HEAD_WIDTH = 128
VOCAB = 65536
BLOCK = 64
LAYERS = 4
CONTEXT_TOKENS = 128
N_SEQ = 2
N_TP = 4


def draw_qkv_weight(key, part):
    group_factor = N_TP
    query_heads = QUERY_HEADS // group_factor
    key_value_heads = KEY_VALUE_HEADS // group_factor
    drawn = jax.random.normal(key, (LAYERS, D, group_factor, query_heads + 2 * key_value_heads, HEAD_WIDTH), jnp.float32) * D ** (-0.5)
    drawn = jnp.clip(drawn, -1.0, 1.0)
    return drawn.reshape(LAYERS, D, group_factor * (query_heads + 2 * key_value_heads) * HEAD_WIDTH).astype(jnp.bfloat16)


def plant(values, key, least, top_value):
    index_at = [jax.random.randint(jax.random.fold_in(key, axis), (), 0, length) for axis, length in enumerate(values.shape)]
    widest = values.shape.index(max(values.shape))
    next_to = index_at[:widest] + [(index_at[widest] + 1) % values.shape[widest]] + index_at[widest + 1:]
    return values.at[tuple(index_at)].set(least).at[tuple(next_to)].set(top_value)


def level_of(stream_key, dims, split, low, top_value):
    loudness, own = 1.0, jax.random.fold_in(stream_key, 6)
    for dim, blocks in split:
        draws = jnp.exp(jax.random.uniform(jax.random.fold_in(own, dim), (blocks,), jnp.float32, low / len(split), top_value / len(split)))
        loudness = loudness * jnp.repeat(draws, dims[dim] // blocks).reshape([-1 if axis == dim else 1 for axis in range(len(dims))])
    return loudness


def cumulative_ranks(count, lean):
    portions = [(1 << 20) // math.isqrt(standing ** lean) + 1 for standing in range(1, count + 1)]
    scale = 1 + sum(portions) // (1 << 30)
    return np.cumsum(np.array([max(1, weight // scale) for weight in portions]))


def skewed_ids(own_key, extent, amount, lean):
    grid = cumulative_ranks(amount, lean)
    pick = jax.random.randint(jax.random.fold_in(own_key, 1), extent, 0, int(grid[amount - 1]))
    grade = jnp.searchsorted(jnp.asarray(grid, jnp.int32), pick, side="right")
    return jax.random.permutation(jax.random.fold_in(own_key, 2), amount)[grade].astype(jnp.int32)


def bell_draw(stream_key, shape, scale, limit, pieces=(), kind=jnp.bfloat16):
    array = scale * jax.random.normal(stream_key, shape, jnp.float32)
    if pieces:
        array = array * level_of(stream_key, shape, pieces, -0.22, 0.18)
    return jnp.clip(array, -limit, limit).astype(kind)


def setup_inputs(seed: int = 0) -> dict:
    splits = jax.random.split(jax.random.key(seed), 6)
    return {
        "token_ids": plant(skewed_ids(splits[0], (CONTEXT_TOKENS,), VOCAB, 2), jax.random.fold_in(splits[0], 3), 0, VOCAB - 1).astype(jnp.int32),
        "embed_columns": bell_draw(splits[1], (D, VOCAB), 1.0, 6.0, ((0, 8),)),
        "norm_gain": jnp.clip(1.0 + 0.18 * jax.random.normal(splits[2], (LAYERS, D), jnp.float32), 0.099609375, 1.8984375).astype(jnp.bfloat16),
        "qkv_weight": draw_qkv_weight(jax.random.fold_in(splits[5], 71), 0),
        "out_weight": bell_draw(splits[4], (LAYERS, D, QUERY_HEADS * HEAD_WIDTH), (QUERY_HEADS * HEAD_WIDTH) ** -0.5, 0.125, ((0, 4), (1, 2), (2, 4))),
    }


EPS = 1e-05
ROPE_BASE = 500000.0
MASKED = -1e+30

def rope_tables(positions, head_size):
    half_width = head_size // 2
    inverse_freq = ROPE_BASE ** (-jnp.arange(half_width).astype(jnp.float32) * (2.0 / head_size))
    angles = positions.astype(jnp.float32)[:, None] * inverse_freq[None, :]
    return (jnp.cos(angles), jnp.sin(angles))

def rotate_half(heads, cosine_table, sine_values):
    half_width = heads.shape[-1] // 2
    first_half = heads[..., :half_width]
    second = heads[..., half_width:]
    cosine_table = cosine_table[:, None, :]
    sine_values = sine_values[:, None, :]
    return jnp.concatenate([first_half * cosine_table - second * sine_values, second * cosine_table + first_half * sine_values], axis=-1)

def norm_rows(row_block, gain_row):
    values = row_block.astype(jnp.float32)
    inverse_rms = lax.rsqrt(lax.optimization_barrier(jnp.mean(values * values, axis=-1, keepdims=True)) + EPS)
    return (values * inverse_rms * gain_row.astype(jnp.float32)[None, :]).astype(jnp.bfloat16)

def reference(token_ids, embed_columns, norm_gain, qkv_weight, out_weight):
    group_factor = N_SEQ
    block_row_slice = BLOCK
    query_heads = QUERY_HEADS // N_TP
    key_value_heads = KEY_VALUE_HEADS // N_TP
    repeat_heads = QUERY_HEADS // KEY_VALUE_HEADS
    hidden = jnp.take(embed_columns, token_ids, axis=1).T
    positions = jnp.arange(CONTEXT_TOKENS).astype(jnp.int32)
    cosine_table, sine_values = rope_tables(positions, HEAD_WIDTH)
    row_ids = jnp.arange(block_row_slice)[None, :, None]
    column = jnp.arange(2 * block_row_slice)[None, None, :]
    group_ids = jnp.arange(group_factor)[:, None, None]
    allowed = jnp.where(column < block_row_slice, group_ids > 0, column - block_row_slice <= row_ids)
    states = []
    for layer_index in range(LAYERS):
        normed = norm_rows(hidden, norm_gain[layer_index])
        projected_rows = jnp.dot(normed, qkv_weight[layer_index], preferred_element_type=jnp.float32)
        projected_rows = projected_rows.reshape(CONTEXT_TOKENS, N_TP, query_heads + 2 * key_value_heads, HEAD_WIDTH)
        query_rows = rotate_half(projected_rows[:, :, :query_heads].reshape(CONTEXT_TOKENS, QUERY_HEADS, HEAD_WIDTH), cosine_table, sine_values).astype(jnp.bfloat16)
        key_head_rows = rotate_half(projected_rows[:, :, query_heads:query_heads + key_value_heads].reshape(CONTEXT_TOKENS, KEY_VALUE_HEADS, HEAD_WIDTH), cosine_table, sine_values).astype(jnp.bfloat16)
        value_head_rows = projected_rows[:, :, query_heads + key_value_heads:].reshape(CONTEXT_TOKENS, KEY_VALUE_HEADS, HEAD_WIDTH).astype(jnp.bfloat16)
        key_head_rows = key_head_rows.reshape(group_factor, block_row_slice, KEY_VALUE_HEADS, HEAD_WIDTH)
        value_head_rows = value_head_rows.reshape(group_factor, block_row_slice, KEY_VALUE_HEADS, HEAD_WIDTH)
        both_keys = jnp.concatenate([jnp.broadcast_to(key_head_rows[:1], key_head_rows.shape), key_head_rows], axis=1)
        both_values = jnp.concatenate([jnp.broadcast_to(value_head_rows[:1], value_head_rows.shape), value_head_rows], axis=1)
        query_groups = query_rows.reshape(group_factor, block_row_slice, KEY_VALUE_HEADS, repeat_heads, HEAD_WIDTH).astype(jnp.float32)
        scores = jnp.einsum('grkph,gckh->gkprc', query_groups, both_keys.astype(jnp.float32)) * HEAD_WIDTH ** (-0.5)
        scores = jnp.where(allowed[:, None, None], scores, MASKED)
        weights = jax.nn.softmax(scores, axis=-1).astype(jnp.bfloat16)
        attended = jnp.einsum('gkprc,gckh->grkph', weights.astype(jnp.float32), both_values.astype(jnp.float32)).astype(jnp.bfloat16)
        attended = attended.reshape(CONTEXT_TOKENS, N_TP, query_heads * HEAD_WIDTH)
        out_heads = out_weight[layer_index].reshape(D, N_TP, query_heads * HEAD_WIDTH)
        partial_value = jnp.einsum('rtc,dtc->trd', attended.astype(jnp.float32), out_heads.astype(jnp.float32)).astype(jnp.bfloat16)
        partial_value = lax.optimization_barrier(partial_value)
        summed = lax.optimization_barrier(jnp.sum(partial_value.astype(jnp.float32), axis=0))
        hidden = (hidden.astype(jnp.float32) + summed).astype(jnp.bfloat16)
        states.append(hidden)
    return jnp.stack(states)
```

```python
import functools

import jax
import jax.numpy as jnp
import numpy as np
from jax import lax
from jax.experimental import pallas as pl
from jax.experimental.pallas import tpu as pltpu
from jax.sharding import PartitionSpec as P

QUERY_HEADS = 16
KEY_VALUE_HEADS = 8
HEAD_WIDTH = 128

EPS = 1e-05
ROPE_BASE = 500000.0
MASKED = -1e30
LANES = 128
AXES = ("seq", "section", "tp")


def rope_tables(positions, head_size):
    half_width = head_size // 2
    inverse_freq = ROPE_BASE ** (-jnp.arange(half_width).astype(jnp.float32) * (2.0 / head_size))
    angles = positions.astype(jnp.float32)[:, None] * inverse_freq[None, :]
    return (jnp.cos(angles), jnp.sin(angles))


def full_rope_tables(count, head_size):
    half_width = head_size // 2
    exponents = -np.arange(half_width).astype(np.float32) * np.float32(2.0 / head_size)
    inverse_freq = np.float32(ROPE_BASE) ** exponents
    angles = np.arange(count).astype(np.float32)[:, None] * inverse_freq[None, :]
    cosine, sine = np.cos(angles), np.sin(angles)
    return (
        np.concatenate([cosine, cosine], axis=1).astype(np.float32),
        np.concatenate([-sine, sine], axis=1).astype(np.float32),
    )


VMEM = pl.BlockSpec(memory_space=pltpu.VMEM)
SMEM = pl.BlockSpec(memory_space=pltpu.SMEM)
ANY = pl.BlockSpec(memory_space=pl.ANY)


def lookup_kernel(ids_smem, ids_row, table, out, strips, onehot, sems):
    features, _ = table.shape
    count = ids_row.shape[1]

    def start(i, _):
        first = pl.multiple_of((ids_smem[i] // LANES) * LANES, LANES)
        pltpu.make_async_copy(
            table.at[:, pl.ds(first, LANES)],
            strips.at[:, pl.ds(pl.multiple_of(i * LANES, LANES), LANES)],
            sems.at[i],
        ).start()
        return 0

    lax.fori_loop(0, count, start, 0)
    lanes = lax.rem(ids_row[...], LANES)
    group = 8
    acc = jnp.zeros((features, count), jnp.float32)
    wide = group * LANES
    rows = lax.broadcasted_iota(jnp.int32, (wide, count), 0)
    target = lax.broadcasted_iota(jnp.int32, (1, count), 1) * LANES + lanes
    for g in range(count // group):
        onehot[g] = jnp.where(rows + g * wide == target, 1.0, 0.0).astype(jnp.bfloat16)
    for g in range(count // group):
        for i in range(g * group, (g + 1) * group):
            pltpu.make_async_copy(
                table.at[:, pl.ds(0, LANES)],
                strips.at[:, pl.ds(i * LANES, LANES)],
                sems.at[i],
            ).wait()
        acc = acc + jnp.dot(
            strips[:, g * wide : (g + 1) * wide], onehot[g], preferred_element_type=jnp.float32
        )
    out[...] = acc.T.astype(jnp.bfloat16)


def lookup(ids, table):
    count, features = ids.shape[0], table.shape[0]
    return pl.pallas_call(
        lookup_kernel,
        out_shape=jax.ShapeDtypeStruct((count, features), jnp.bfloat16),
        in_specs=[SMEM, VMEM, ANY],
        out_specs=VMEM,
        scratch_shapes=[
            pltpu.VMEM((features, count * LANES), jnp.bfloat16),
            pltpu.VMEM((count // 8, 8 * LANES, count), jnp.bfloat16),
            pltpu.SemaphoreType.DMA((count,)),
        ],
        name="lookup",
    )(ids, ids.reshape(1, count), table)


def project_kernel(place, *refs, ways):
    pieces, (gain, weight, mine, sent, kept, w_buf, sems) = refs[:ways], refs[ways:]
    rank = place[0]
    width = pieces[0].shape[1]
    firsts = []
    for k in range(ways):
        first = pl.multiple_of(lax.rem(rank + ways - k, ways) * width, width)
        firsts.append(first)
        pltpu.make_async_copy(weight.at[0, pl.ds(first, width), :], w_buf.at[k], sems.at[k]).start()
    squares = None
    acc = None
    for k in range(ways):
        values = pieces[k][...].astype(jnp.float32)
        square = jnp.sum(values * values, axis=1, keepdims=True)
        squares = square if squares is None else squares + square
        scaled = (values * gain[:, pl.ds(firsts[k], width)]).astype(jnp.bfloat16)
        pltpu.make_async_copy(weight.at[0, pl.ds(0, width), :], w_buf.at[k], sems.at[k]).wait()
        part = jnp.dot(scaled, w_buf[k], preferred_element_type=jnp.float32)
        acc = part if acc is None else acc + part
    cols = acc.shape[1]
    mine[:, :cols] = acc
    mine[:, cols:] = jnp.broadcast_to(squares, (acc.shape[0], LANES))
    sent[:, :cols] = acc.astype(jnp.bfloat16)
    high = squares.astype(jnp.bfloat16)
    low = squares - high.astype(jnp.float32)
    lane = lax.broadcasted_iota(jnp.int32, (acc.shape[0], LANES), 1)
    sent[:, cols:] = jnp.where(lane < LANES // 2, high.astype(jnp.float32), low).astype(jnp.bfloat16)
    kept[...] = pieces[0][...]


def project(place, pieces, gain, weight):
    rows, width = pieces[0].shape
    ways = len(pieces)
    cols = weight.shape[2]
    return pl.pallas_call(
        functools.partial(project_kernel, ways=ways),
        out_shape=[
            jax.ShapeDtypeStruct((rows, cols + LANES), jnp.float32),
            jax.ShapeDtypeStruct((rows, cols + LANES), jnp.bfloat16),
            jax.ShapeDtypeStruct((rows, width), jnp.bfloat16),
        ],
        in_specs=[SMEM] + [VMEM] * ways + [VMEM, ANY],
        out_specs=[VMEM] * 3,
        scratch_shapes=[
            pltpu.VMEM((ways, width, cols), jnp.bfloat16),
            pltpu.SemaphoreType.DMA((ways,)),
        ],
        name="project",
    )(place, *pieces, gain, weight)


def attended_heads(total, inverse, cosine, sine, block, query_heads, key_value_heads, features):
    rows = total.shape[0]
    repeat = query_heads // key_value_heads

    def head(i):
        return total[:, i * HEAD_WIDTH : (i + 1) * HEAD_WIDTH] * inverse

    def rotated(i):
        values = head(i)
        turned = values * cosine + pltpu.roll(values, HEAD_WIDTH // 2, 1) * sine
        return turned.astype(jnp.bfloat16)

    row = lax.broadcasted_iota(jnp.int32, (rows, rows), 0)
    col = lax.broadcasted_iota(jnp.int32, (rows, rows), 1)
    row_block, col_block = row // block, col // block
    allowed = ((row_block == col_block) & (col <= row)) | ((col_block == 0) & (row_block > 0))
    keys = [rotated(query_heads + j) for j in range(key_value_heads)]
    held = [head(query_heads + key_value_heads + j).astype(jnp.bfloat16) for j in range(key_value_heads)]
    results = []
    for i in range(query_heads):
        scores = lax.dot_general(
            rotated(i), keys[i // repeat], (((1,), (1,)), ((), ())), preferred_element_type=jnp.float32
        ) * HEAD_WIDTH ** (-0.5)
        scores = jnp.where(allowed, scores, MASKED)
        top = jnp.max(scores, axis=1, keepdims=True)
        powers = jnp.exp(scores - top)
        weights = (powers / jnp.sum(powers, axis=1, keepdims=True)).astype(jnp.bfloat16)
        results.append(
            jnp.dot(weights, held[i // repeat], preferred_element_type=jnp.float32).astype(jnp.bfloat16)
        )
    return jnp.concatenate(results, axis=1)


def attend_kernel(place, mine, got, cosine, sine, weight, *refs, ways, block, features, heads):
    outs, (w_buf, sems) = refs[:ways], refs[ways:]
    rank = place[0]
    width = w_buf.shape[1]
    for k in range(ways):
        first = pl.multiple_of(lax.rem(rank + k, ways) * width, width)
        pltpu.make_async_copy(weight.at[0, pl.ds(first, width), :], w_buf.at[k], sems.at[k]).start()
    cols = mine.shape[1] - LANES
    squares = (
        mine[:, cols : cols + 1]
        + got[:, cols : cols + 1].astype(jnp.float32)
        + got[:, cols + LANES // 2 : cols + LANES // 2 + 1].astype(jnp.float32)
    )
    inverse = lax.rsqrt(squares / features + EPS)
    total = mine[:, :cols] + got[:, :cols].astype(jnp.float32)
    attended = attended_heads(total, inverse, cosine[...], sine[...], block, *heads, features)
    for n in range(ways):
        k = (n + 1) % ways
        pltpu.make_async_copy(weight.at[0, pl.ds(0, width), :], w_buf.at[k], sems.at[k]).wait()
        part = lax.dot_general(
            attended, w_buf[k], (((1,), (1,)), ((), ())), preferred_element_type=jnp.float32
        )
        outs[k][...] = part.astype(outs[k].dtype)


def attend(place, mine, got, cosine, sine, weight, ways, block, features, heads):
    rows = mine.shape[0]
    width = weight.shape[1] // ways
    return pl.pallas_call(
        functools.partial(attend_kernel, ways=ways, block=block, features=features, heads=heads),
        out_shape=[
            jax.ShapeDtypeStruct((rows, width), jnp.float32 if k == 0 else jnp.bfloat16)
            for k in range(ways)
        ],
        in_specs=[SMEM] + [VMEM] * 4 + [ANY],
        out_specs=[VMEM] * ways,
        scratch_shapes=[
            pltpu.VMEM((ways, width, weight.shape[2]), jnp.bfloat16),
            pltpu.SemaphoreType.DMA((ways,)),
        ],
        name="attend",
    )(place, mine, got, cosine, sine, weight)


def combine_kernel(own, *refs, ways):
    parts, (residual, out) = refs[: ways - 1], refs[ways - 1 :]
    total = own[...]
    for part in parts:
        total = total + part[...].astype(jnp.float32)
    out[...] = (residual[...].astype(jnp.float32) + total).astype(jnp.bfloat16)


def combine(own, parts, residual):
    return pl.pallas_call(
        functools.partial(combine_kernel, ways=len(parts) + 1),
        out_shape=jax.ShapeDtypeStruct(own.shape, jnp.bfloat16),
        in_specs=[VMEM] * (len(parts) + 2),
        out_specs=VMEM,
        name="combine",
    )(own, *parts, residual)


def stationary_body(token_ids, embed_columns, norm_gain, qkv_weight, out_weight):
    seq_count = lax.axis_size("seq")
    sections = lax.axis_size("section")
    ways = lax.axis_size("tp")
    s, c, t = lax.axis_index("seq"), lax.axis_index("section"), lax.axis_index("tp")
    block = token_ids.shape[0]
    rows = block * seq_count
    width = embed_columns.shape[0]
    half = qkv_weight.shape[1]
    features = half * seq_count
    heads = (QUERY_HEADS // ways, KEY_VALUE_HEADS // ways)

    def at(seq, section, tp):
        return (seq * sections + section) * ways + tp

    def moved(value, pairs):
        return lax.ppermute(value, AXES, pairs)

    place = jnp.reshape(t, (1,)).astype(jnp.int32)
    gain = lax.dynamic_slice_in_dim(norm_gain, s * half, half, axis=1).astype(jnp.float32)
    cosine, sine = (jnp.asarray(table) for table in full_rope_tables(rows, HEAD_WIDTH))

    other_ids = lax.ppermute(token_ids, "seq", [(0, 1), (1, 0)])
    own_rows = lookup(token_ids, embed_columns)
    other_rows = lookup(other_ids, embed_columns)
    looked = jnp.where(
        s == 0,
        jnp.concatenate([own_rows, other_rows], axis=0),
        jnp.concatenate([other_rows, own_rows], axis=0),
    )
    server = [0, 2, 1, 3]
    pieces = []
    for k in range(ways):
        pairs = []
        for s1 in range(seq_count):
            for t1 in range(ways):
                b = s1 * ways + (t1 - k) % ways
                pairs.append((at(b % seq_count, server[t1], b // seq_count), at(s1, 0, t1)))
        pieces.append(moved(looked, pairs))

    state = jnp.zeros((rows, width), jnp.bfloat16)
    for layer in range(sections):
        mine, sent, residual = project(place, pieces, gain, qkv_weight)
        got = moved(sent, [(at(s1, layer, t1), at(1 - s1, layer, t1)) for s1 in range(2) for t1 in range(ways)])
        outs = attend(place, mine, got, cosine, sine, out_weight, ways, block, features, heads)
        order = [2, 1, 3]
        parts = {
            k: moved(
                outs[k],
                [(at(s1, layer, t1), at(s1, layer, (t1 + k) % ways)) for s1 in range(2) for t1 in range(ways)],
            )
            for k in order
        }
        fresh = combine(outs[0], [parts[k] for k in range(1, ways)], residual)
        state = jnp.where(c == layer, fresh, state)
        if layer + 1 < sections:
            pieces = [
                moved(
                    fresh,
                    [
                        (at(s1, layer, t1), at(s1, layer + 1, (t1 + k) % ways))
                        for s1 in range(2)
                        for t1 in range(ways)
                    ],
                )
                for k in range(ways)
            ]

    arrived = []
    for m in range(2):
        chosen = lax.dynamic_slice_in_dim(state, lax.rem(t + m, 2) * block, block, axis=0)
        pairs = []
        for section in range(sections):
            for s2 in range(seq_count):
                for t2 in range(ways):
                    pairs.append((at(s2, section, t2), at((t2 + m) % 2, section, 2 * s2 + t2 // 2)))
        arrived.append(moved(chosen, pairs))
    result = jnp.where(
        s == 0,
        jnp.concatenate(arrived, axis=1),
        jnp.concatenate(arrived[::-1], axis=1),
    )
    return result[None]


def passed_along(value, axis, steps):
    count = lax.axis_size(axis)
    leading, last = (max(0, -steps), min(count, count - steps))
    return lax.ppermute(value, axis, [(source, source + steps) for source in range(leading, last)])


def from_root(value, axis, root):
    mine = lax.axis_index(axis) == root
    return lax.psum(jnp.where(mine, value, jnp.zeros_like(value)), axis)


def rotate_half(heads, cosine_table, sine_values):
    half_width = heads.shape[-1] // 2
    first_half = heads[..., :half_width]
    second = heads[..., half_width:]
    cosine_table = cosine_table[:, None, :]
    sine_values = sine_values[:, None, :]
    return jnp.concatenate(
        [
            first_half * cosine_table - second * sine_values,
            second * cosine_table + first_half * sine_values,
        ],
        axis=-1,
    )


def norm_rows(row_block, gain_row):
    values = row_block.astype(jnp.float32)
    inverse_rms = lax.rsqrt(jnp.mean(values * values, axis=-1, keepdims=True) + EPS)
    return (values * inverse_rms * gain_row[None, :]).astype(jnp.bfloat16)


def gathered_project(full_rows, gain_row, qkv_full, positions, query_heads, key_value_heads):
    row_count = full_rows.shape[0]
    normed = norm_rows(full_rows, gain_row)
    projected_rows = jnp.dot(normed, qkv_full, preferred_element_type=jnp.float32)
    projected_rows = projected_rows.reshape(row_count, query_heads + 2 * key_value_heads, HEAD_WIDTH)
    cosine_table, sine_values = rope_tables(positions, HEAD_WIDTH)
    query_rows = rotate_half(projected_rows[:, :query_heads], cosine_table, sine_values)
    key_head_rows = rotate_half(
        projected_rows[:, query_heads : query_heads + key_value_heads], cosine_table, sine_values
    )
    value_head_rows = projected_rows[:, query_heads + key_value_heads :]
    return tuple(v.astype(jnp.bfloat16) for v in (query_rows, key_head_rows, value_head_rows))


def gathered_attend(query_rows, key_head_rows, value_head_rows, allowed):
    row_count, query_heads, head_size = query_rows.shape
    key_value_heads = key_head_rows.shape[1]
    query_groups = query_rows.reshape(row_count, key_value_heads, query_heads // key_value_heads, head_size)
    scores = jnp.einsum(
        "rkph,ckh->kprc", query_groups, key_head_rows, preferred_element_type=jnp.float32
    ) * head_size ** (-0.5)
    scores = jnp.where(allowed[None, None], scores, MASKED)
    weights = jax.nn.softmax(scores, axis=-1).astype(jnp.bfloat16)
    attended = jnp.einsum("kprc,ckh->rkph", weights, value_head_rows, preferred_element_type=jnp.float32)
    return attended.reshape(row_count, query_heads * head_size).astype(jnp.bfloat16)


def gathered_combine(current, attended, out_full):
    partial_value = lax.dot_general(
        attended, out_full, (((1,), (1,)), ((), ())), preferred_element_type=jnp.float32
    )
    summed = lax.psum_scatter(
        partial_value.astype(jnp.bfloat16), "tp", scatter_dimension=1, tiled=True
    ).astype(jnp.float32)
    return (current.astype(jnp.float32) + summed).astype(jnp.bfloat16)


def gathered_body(token_ids, embed_columns, norm_gain, qkv_weight, out_weight):
    seq_count = lax.axis_size("seq")
    section_count = lax.axis_size("section")
    tensor_parallel_count = lax.axis_size("tp")
    group_index = lax.axis_index("seq")
    section_index = lax.axis_index("section")
    block_row_slice = token_ids.shape[0]
    feature_cols = embed_columns.shape[0] * seq_count
    query_heads = QUERY_HEADS // tensor_parallel_count
    key_value_heads = KEY_VALUE_HEADS // tensor_parallel_count
    every_id = lax.all_gather(token_ids, "seq", axis=0, tiled=True)
    looked = jnp.take(embed_columns, every_id, axis=1)
    current = lax.all_to_all(looked, "seq", split_axis=1, concat_axis=0, tiled=True).T
    qkv_full = lax.all_gather(qkv_weight, "seq", axis=1, tiled=True)[0]
    out_full = lax.all_gather(out_weight, "seq", axis=1, tiled=True)[0]
    gain_row = norm_gain[0].astype(jnp.float32)
    outputs = jnp.zeros((block_row_slice, feature_cols), jnp.bfloat16)
    row_ids = jnp.arange(block_row_slice)[:, None]
    column = jnp.arange(2 * block_row_slice)[None, :]
    positions = group_index * block_row_slice + jnp.arange(block_row_slice)
    allowed = jnp.where(column < block_row_slice, group_index > 0, column - block_row_slice <= row_ids)
    for step_number in range(section_count):
        full_rows = lax.all_gather(current, "tp", axis=1, tiled=True)
        query_rows, key_head_rows, value_head_rows = gathered_project(
            full_rows, gain_row, qkv_full, positions, query_heads, key_value_heads
        )
        anchor_heads = from_root(key_head_rows, "seq", 0)
        anchor_values = from_root(value_head_rows, "seq", 0)
        both_keys = jnp.concatenate([anchor_heads, key_head_rows], axis=0)
        both_values = jnp.concatenate([anchor_values, value_head_rows], axis=0)
        attended = gathered_attend(query_rows, both_keys, both_values, allowed)
        new_rows = gathered_combine(current, attended, out_full)
        outputs = jnp.where(section_index == step_number, new_rows, outputs)
        if step_number + 1 < section_count:
            current = passed_along(new_rows, "section", 1)
    return outputs[None]


def solution(mesh):
    placed = (
        P("seq"),
        P(("tp", "seq"), None),
        P("section", None),
        P("section", "seq", "tp"),
        P("section", "seq", "tp"),
    )
    sizes = mesh.shape
    small = sizes["seq"] == 2 and sizes["tp"] == 4 and sizes["section"] == 4
    return jax.shard_map(
        stationary_body if small else gathered_body,
        mesh=mesh,
        in_specs=placed,
        out_specs=P("section", "seq", "tp"),
        check_vma=False,
    )
```

```python
import functools

import jax
import jax.numpy as jnp
import numpy as np
from jax import lax
from jax.experimental import pallas as pl
from jax.experimental.pallas import tpu as pltpu
from jax.sharding import PartitionSpec as P

QUERY_HEADS = 16
KEY_VALUE_HEADS = 8
HEAD_WIDTH = 128

EPS = 1e-05
ROPE_BASE = 500000.0
MASKED = -1e30
LANES = 128
AXES = ("seq", "section", "tp")


def rope_tables(positions, head_size):
    half_width = head_size // 2
    inverse_freq = ROPE_BASE ** (-jnp.arange(half_width).astype(jnp.float32) * (2.0 / head_size))
    angles = positions.astype(jnp.float32)[:, None] * inverse_freq[None, :]
    return (jnp.cos(angles), jnp.sin(angles))


def full_rope_tables(count, head_size):
    half_width = head_size // 2
    exponents = -np.arange(half_width).astype(np.float32) * np.float32(2.0 / head_size)
    inverse_freq = np.float32(ROPE_BASE) ** exponents
    angles = np.arange(count).astype(np.float32)[:, None] * inverse_freq[None, :]
    cosine, sine = np.cos(angles), np.sin(angles)
    return (
        np.concatenate([cosine, cosine], axis=1).astype(np.float32),
        np.concatenate([-sine, sine], axis=1).astype(np.float32),
    )


VMEM = pl.BlockSpec(memory_space=pltpu.VMEM)
SMEM = pl.BlockSpec(memory_space=pltpu.SMEM)
ANY = pl.BlockSpec(memory_space=pl.ANY)


def lookup_kernel(active, ids_smem, ids_row, table, out, strips, onehot, sems):
    @pl.when(active[0] == 1)
    def _():
        read_columns(ids_smem, ids_row, table, out, strips, onehot, sems)


def read_columns(ids_smem, ids_row, table, out, strips, onehot, sems):
    features, _ = table.shape
    count = ids_row.shape[1]

    def start(i, _):
        first = pl.multiple_of((ids_smem[i] // LANES) * LANES, LANES)
        pltpu.make_async_copy(
            table.at[:, pl.ds(first, LANES)],
            strips.at[:, pl.ds(pl.multiple_of(i * LANES, LANES), LANES)],
            sems.at[i],
        ).start()
        return 0

    lax.fori_loop(0, count, start, 0)
    lanes = lax.rem(ids_row[...], LANES)
    group = 8
    acc = jnp.zeros((features, count), jnp.float32)
    wide = group * LANES
    rows = lax.broadcasted_iota(jnp.int32, (wide, count), 0)
    target = lax.broadcasted_iota(jnp.int32, (1, count), 1) * LANES + lanes
    for g in range(count // group):
        onehot[g] = jnp.where(rows + g * wide == target, 1.0, 0.0).astype(jnp.bfloat16)
    for g in range(count // group):
        for i in range(g * group, (g + 1) * group):
            pltpu.make_async_copy(
                table.at[:, pl.ds(0, LANES)],
                strips.at[:, pl.ds(i * LANES, LANES)],
                sems.at[i],
            ).wait()
        acc = acc + jnp.dot(
            strips[:, g * wide : (g + 1) * wide], onehot[g], preferred_element_type=jnp.float32
        )
    out[...] = acc.T.astype(jnp.bfloat16)


def lookup(active, ids, table):
    count, features = ids.shape[0], table.shape[0]
    return pl.pallas_call(
        lookup_kernel,
        out_shape=jax.ShapeDtypeStruct((count, features), jnp.bfloat16),
        in_specs=[SMEM, SMEM, VMEM, ANY],
        out_specs=VMEM,
        scratch_shapes=[
            pltpu.VMEM((features, count * LANES), jnp.bfloat16),
            pltpu.VMEM((count // 8, 8 * LANES, count), jnp.bfloat16),
            pltpu.SemaphoreType.DMA((count,)),
        ],
        name="lookup",
        compiler_params=pltpu.CompilerParams(vmem_limit_bytes=16 << 20),
    )(active, ids, ids.reshape(1, count), table)


def send_order(ways):
    return sorted(range(ways), key=lambda k: -min(k, ways - k))


def whole_piece(rank, k, ways, parts):
    if len(parts) == 1:
        return parts[0][...]
    even = lax.rem(rank + ways - k, 2) == 0
    first, second = parts[0][...], parts[1][...]
    return jnp.concatenate([jnp.where(even, first, second), jnp.where(even, second, first)], axis=0)


def project_kernel(place, *refs, ways, split):
    pieces, (gain, weight, near, far, kept) = refs[: ways * split], refs[ways * split :]
    rank = place[0]
    width = pieces[0].shape[1]
    squares = None
    acc = None
    for n, k in enumerate(send_order(ways)):
        piece = whole_piece(rank, k, ways, pieces[n * split : (n + 1) * split])
        if k == 0:
            kept[...] = piece
        values = piece.astype(jnp.float32)
        square = jnp.sum(values * values, axis=1, keepdims=True)
        squares = square if squares is None else squares + square
        first = pl.multiple_of(lax.rem(rank + ways - k, ways) * width, width)
        scaled = (values * gain[:, pl.ds(first, width)]).astype(jnp.bfloat16)
        part = jnp.dot(scaled, weight[0, pl.ds(first, width), :], preferred_element_type=jnp.float32)
        acc = part if acc is None else acc + part
    cols = acc.shape[1]
    near[:, :cols] = acc
    near[:, cols:] = jnp.broadcast_to(squares, (acc.shape[0], LANES))
    far[:, :cols] = acc.astype(jnp.bfloat16)
    high = squares.astype(jnp.bfloat16)
    low = squares - high.astype(jnp.float32)
    lane = lax.broadcasted_iota(jnp.int32, (acc.shape[0], LANES), 1)
    far[:, cols:] = jnp.where(lane < LANES // 2, high.astype(jnp.float32), low).astype(jnp.bfloat16)


def project(place, pieces, gain, weight, ways):
    split = len(pieces) // ways
    rows, width = pieces[0].shape[0] * split, pieces[0].shape[1]
    cols = weight.shape[2]
    return pl.pallas_call(
        functools.partial(project_kernel, ways=ways, split=split),
        out_shape=[
            jax.ShapeDtypeStruct((rows, cols + LANES), jnp.float32),
            jax.ShapeDtypeStruct((rows, cols + LANES), jnp.bfloat16),
            jax.ShapeDtypeStruct((rows, width), jnp.bfloat16),
        ],
        in_specs=[SMEM] + [VMEM] * (len(pieces) + 2),
        out_specs=[VMEM] * 3,
        name="project",
        compiler_params=pltpu.CompilerParams(vmem_limit_bytes=12 << 20),
    )(place, *pieces, gain, weight)


def stage_kernel(weight, after, out, sem):
    copy = pltpu.make_async_copy(weight, out, sem)
    copy.start()
    copy.wait()


def stage(weight, after):
    return pl.pallas_call(
        stage_kernel,
        out_shape=jax.ShapeDtypeStruct(weight.shape, weight.dtype),
        in_specs=[ANY, ANY],
        out_specs=VMEM,
        scratch_shapes=[pltpu.SemaphoreType.DMA],
        name="stage",
        compiler_params=pltpu.CompilerParams(vmem_limit_bytes=12 << 20),
    )(weight, after)


def attended_heads(total, inverse, cosine, sine, block, query_heads, key_value_heads, features):
    rows = total.shape[0]
    repeat = query_heads // key_value_heads

    def head(i):
        return total[:, i * HEAD_WIDTH : (i + 1) * HEAD_WIDTH] * inverse

    def rotated(i):
        values = head(i)
        turned = values * cosine + pltpu.roll(values, HEAD_WIDTH // 2, 1) * sine
        return turned.astype(jnp.bfloat16)

    row = lax.broadcasted_iota(jnp.int32, (rows, rows), 0)
    col = lax.broadcasted_iota(jnp.int32, (rows, rows), 1)
    row_block, col_block = row // block, col // block
    allowed = ((row_block == col_block) & (col <= row)) | ((col_block == 0) & (row_block > 0))
    keys = [rotated(query_heads + j) for j in range(key_value_heads)]
    held = [head(query_heads + key_value_heads + j).astype(jnp.bfloat16) for j in range(key_value_heads)]
    results = []
    for i in range(query_heads):
        scores = lax.dot_general(
            rotated(i), keys[i // repeat], (((1,), (1,)), ((), ())), preferred_element_type=jnp.float32
        ) * HEAD_WIDTH ** (-0.5)
        scores = jnp.where(allowed, scores, MASKED)
        top = jnp.max(scores, axis=1, keepdims=True)
        powers = jnp.exp(scores - top)
        weights = (powers / jnp.sum(powers, axis=1, keepdims=True)).astype(jnp.bfloat16)
        results.append(
            jnp.dot(weights, held[i // repeat], preferred_element_type=jnp.float32).astype(jnp.bfloat16)
        )
    return jnp.concatenate(results, axis=1)


def attend_kernel(place, got, mine, cosine, sine, weight, *outs, ways, block, features, heads):
    rank = place[0]
    width = weight.shape[1] // ways
    cols = mine.shape[1] - LANES
    squares = (
        mine[:, cols : cols + 1]
        + got[:, cols : cols + 1].astype(jnp.float32)
        + got[:, cols + LANES // 2 : cols + LANES // 2 + 1].astype(jnp.float32)
    )
    inverse = lax.rsqrt(squares / features + EPS)
    total = mine[:, :cols] + got[:, :cols].astype(jnp.float32)
    attended = attended_heads(total, inverse, cosine[...], sine[...], block, *heads, features)
    for k in range(ways):
        first = pl.multiple_of(lax.rem(rank + k, ways) * width, width)
        part = lax.dot_general(
            attended,
            weight[0, pl.ds(first, width), :],
            (((1,), (1,)), ((), ())),
            preferred_element_type=jnp.float32,
        )
        outs[k][...] = part.astype(outs[k].dtype)


def attend(place, got, mine, cosine, sine, weight, ways, block, features, heads):
    rows = mine.shape[0]
    width = weight.shape[1] // ways
    return pl.pallas_call(
        functools.partial(attend_kernel, ways=ways, block=block, features=features, heads=heads),
        out_shape=[
            jax.ShapeDtypeStruct((rows, width), jnp.bfloat16) for _ in range(ways)
        ],
        in_specs=[SMEM] + [VMEM] * 5,
        out_specs=[VMEM] * ways,
        name="attend",
        compiler_params=pltpu.CompilerParams(vmem_limit_bytes=12 << 20),
    )(place, got, mine, cosine, sine, weight)


def combine_kernel(*refs, ways):
    parts, (residual, out) = refs[:ways], refs[ways:]
    total = parts[0][...].astype(jnp.float32)
    for part in parts[1:]:
        total = total + part[...].astype(jnp.float32)
    out[...] = (residual[...].astype(jnp.float32) + total).astype(jnp.bfloat16)


def combine(parts, residual):
    return pl.pallas_call(
        functools.partial(combine_kernel, ways=len(parts)),
        out_shape=jax.ShapeDtypeStruct(residual.shape, jnp.bfloat16),
        in_specs=[VMEM] * (len(parts) + 1),
        out_specs=VMEM,
        name="combine",
        compiler_params=pltpu.CompilerParams(vmem_limit_bytes=4 << 20),
    )(*parts, residual)


def stationary_body(token_ids, embed_columns, norm_gain, qkv_weight, out_weight):
    seq_count = lax.axis_size("seq")
    sections = lax.axis_size("section")
    ways = lax.axis_size("tp")
    s, c, t = lax.axis_index("seq"), lax.axis_index("section"), lax.axis_index("tp")
    block = token_ids.shape[0]
    rows = block * seq_count
    width = embed_columns.shape[0]
    half = qkv_weight.shape[1]
    features = half * seq_count
    heads = (QUERY_HEADS // ways, KEY_VALUE_HEADS // ways)

    def at(seq, section, tp):
        return (seq * sections + section) * ways + tp

    def moved(value, pairs):
        return lax.ppermute(value, AXES, pairs)

    place = jnp.reshape(t, (1,)).astype(jnp.int32)
    gain = lax.dynamic_slice_in_dim(norm_gain, s * half, half, axis=1).astype(jnp.float32)
    cosine, sine = (jnp.asarray(table) for table in full_rope_tables(rows, HEAD_WIDTH))

    def partner(section):
        return section ^ 1

    everywhere = [(s1, t1) for s1 in range(seq_count) for t1 in range(ways)]

    lent = lax.ppermute(out_weight, "section", [(i, partner(i)) for i in range(sections)])

    other_ids = lax.ppermute(token_ids, "seq", [(0, 1), (1, 0)])
    servers = {0: lambda t1: 1, 1: lambda t1: 2 + t1 // 2}
    readers = {0: c == 1, 1: c >= 2}
    arrivals = {}
    for group, ids in enumerate((token_ids, other_ids)):
        looked = lookup(jnp.reshape(readers[group], (1,)).astype(jnp.int32), ids, embed_columns)
        for k in send_order(ways):
            pairs = []
            for s1, t1 in everywhere:
                b = s1 * ways + (t1 - k) % ways
                pairs.append((at(b % seq_count, servers[group](t1), b // seq_count), at(s1, 0, t1)))
            arrivals[k, group] = moved(looked, pairs)
    staged = stage(qkv_weight, looked)
    pieces = [arrivals[k, group] for k in send_order(ways) for group in range(2)]

    state = jnp.zeros((rows, width), jnp.bfloat16)
    for layer in range(sections):
        aside = partner(layer)
        near, far, residual = project(place, pieces, gain, staged, ways)
        got_far = moved(far, [(at(s1, layer, t1), at(1 - s1, aside, t1)) for s1, t1 in everywhere])
        got_near = moved(near, [(at(s1, layer, t1), at(s1, aside, t1)) for s1, t1 in everywhere])
        outs = attend(place, got_far, got_near, cosine, sine, lent, ways, block, features, heads)
        parts = [
            moved(outs[k], [(at(s1, aside, t1), at(s1, layer, (t1 + k) % ways)) for s1, t1 in everywhere])
            for k in send_order(ways)
        ]
        fresh = combine(parts, residual)
        state = jnp.where(c == layer, fresh, state)
        if layer + 1 < sections:
            pieces = [
                moved(fresh, [(at(s1, layer, t1), at(s1, layer + 1, (t1 + k) % ways)) for s1, t1 in everywhere])
                for k in send_order(ways)
            ]

    arrived = []
    for m in range(2):
        chosen = lax.dynamic_slice_in_dim(state, lax.rem(t + m, 2) * block, block, axis=0)
        pairs = []
        for section in range(sections):
            for s2 in range(seq_count):
                for t2 in range(ways):
                    pairs.append((at(s2, section, t2), at((t2 + m) % 2, section, 2 * s2 + t2 // 2)))
        arrived.append(moved(chosen, pairs))
    result = jnp.where(
        s == 0,
        jnp.concatenate(arrived, axis=1),
        jnp.concatenate(arrived[::-1], axis=1),
    )
    return result[None]


def passed_along(value, axis, steps):
    count = lax.axis_size(axis)
    leading, last = (max(0, -steps), min(count, count - steps))
    return lax.ppermute(value, axis, [(source, source + steps) for source in range(leading, last)])


def from_root(value, axis, root):
    mine = lax.axis_index(axis) == root
    return lax.psum(jnp.where(mine, value, jnp.zeros_like(value)), axis)


def rotate_half(heads, cosine_table, sine_values):
    half_width = heads.shape[-1] // 2
    first_half = heads[..., :half_width]
    second = heads[..., half_width:]
    cosine_table = cosine_table[:, None, :]
    sine_values = sine_values[:, None, :]
    return jnp.concatenate(
        [
            first_half * cosine_table - second * sine_values,
            second * cosine_table + first_half * sine_values,
        ],
        axis=-1,
    )


def norm_rows(row_block, gain_row):
    values = row_block.astype(jnp.float32)
    inverse_rms = lax.rsqrt(jnp.mean(values * values, axis=-1, keepdims=True) + EPS)
    return (values * inverse_rms * gain_row[None, :]).astype(jnp.bfloat16)


def gathered_project(full_rows, gain_row, qkv_full, positions, query_heads, key_value_heads):
    row_count = full_rows.shape[0]
    normed = norm_rows(full_rows, gain_row)
    projected_rows = jnp.dot(normed, qkv_full, preferred_element_type=jnp.float32)
    projected_rows = projected_rows.reshape(row_count, query_heads + 2 * key_value_heads, HEAD_WIDTH)
    cosine_table, sine_values = rope_tables(positions, HEAD_WIDTH)
    query_rows = rotate_half(projected_rows[:, :query_heads], cosine_table, sine_values)
    key_head_rows = rotate_half(
        projected_rows[:, query_heads : query_heads + key_value_heads], cosine_table, sine_values
    )
    value_head_rows = projected_rows[:, query_heads + key_value_heads :]
    return tuple(v.astype(jnp.bfloat16) for v in (query_rows, key_head_rows, value_head_rows))


def gathered_attend(query_rows, key_head_rows, value_head_rows, allowed):
    row_count, query_heads, head_size = query_rows.shape
    key_value_heads = key_head_rows.shape[1]
    query_groups = query_rows.reshape(row_count, key_value_heads, query_heads // key_value_heads, head_size)
    scores = jnp.einsum(
        "rkph,ckh->kprc", query_groups, key_head_rows, preferred_element_type=jnp.float32
    ) * head_size ** (-0.5)
    scores = jnp.where(allowed[None, None], scores, MASKED)
    weights = jax.nn.softmax(scores, axis=-1).astype(jnp.bfloat16)
    attended = jnp.einsum("kprc,ckh->rkph", weights, value_head_rows, preferred_element_type=jnp.float32)
    return attended.reshape(row_count, query_heads * head_size).astype(jnp.bfloat16)


def gathered_combine(current, attended, out_full):
    partial_value = lax.dot_general(
        attended, out_full, (((1,), (1,)), ((), ())), preferred_element_type=jnp.float32
    )
    summed = lax.psum_scatter(
        partial_value.astype(jnp.bfloat16), "tp", scatter_dimension=1, tiled=True
    ).astype(jnp.float32)
    return (current.astype(jnp.float32) + summed).astype(jnp.bfloat16)


def gathered_body(token_ids, embed_columns, norm_gain, qkv_weight, out_weight):
    seq_count = lax.axis_size("seq")
    section_count = lax.axis_size("section")
    tensor_parallel_count = lax.axis_size("tp")
    group_index = lax.axis_index("seq")
    section_index = lax.axis_index("section")
    block_row_slice = token_ids.shape[0]
    feature_cols = embed_columns.shape[0] * seq_count
    query_heads = QUERY_HEADS // tensor_parallel_count
    key_value_heads = KEY_VALUE_HEADS // tensor_parallel_count
    every_id = lax.all_gather(token_ids, "seq", axis=0, tiled=True)
    looked = jnp.take(embed_columns, every_id, axis=1)
    current = lax.all_to_all(looked, "seq", split_axis=1, concat_axis=0, tiled=True).T
    qkv_full = lax.all_gather(qkv_weight, "seq", axis=1, tiled=True)[0]
    out_full = lax.all_gather(out_weight, "seq", axis=1, tiled=True)[0]
    gain_row = norm_gain[0].astype(jnp.float32)
    outputs = jnp.zeros((block_row_slice, feature_cols), jnp.bfloat16)
    row_ids = jnp.arange(block_row_slice)[:, None]
    column = jnp.arange(2 * block_row_slice)[None, :]
    positions = group_index * block_row_slice + jnp.arange(block_row_slice)
    allowed = jnp.where(column < block_row_slice, group_index > 0, column - block_row_slice <= row_ids)
    for step_number in range(section_count):
        full_rows = lax.all_gather(current, "tp", axis=1, tiled=True)
        query_rows, key_head_rows, value_head_rows = gathered_project(
            full_rows, gain_row, qkv_full, positions, query_heads, key_value_heads
        )
        anchor_heads = from_root(key_head_rows, "seq", 0)
        anchor_values = from_root(value_head_rows, "seq", 0)
        both_keys = jnp.concatenate([anchor_heads, key_head_rows], axis=0)
        both_values = jnp.concatenate([anchor_values, value_head_rows], axis=0)
        attended = gathered_attend(query_rows, both_keys, both_values, allowed)
        new_rows = gathered_combine(current, attended, out_full)
        outputs = jnp.where(section_index == step_number, new_rows, outputs)
        if step_number + 1 < section_count:
            current = passed_along(new_rows, "section", 1)
    return outputs[None]


def solution(mesh):
    placed = (
        P("seq"),
        P(("tp", "seq"), None),
        P("section", None),
        P("section", "seq", "tp"),
        P("section", "seq", "tp"),
    )
    sizes = mesh.shape
    small = sizes["seq"] == 2 and sizes["tp"] == 4 and sizes["section"] == 4
    return jax.shard_map(
        stationary_body if small else gathered_body,
        mesh=mesh,
        in_specs=placed,
        out_specs=P("section", "seq", "tp"),
        check_vma=False,
    )
```

```python
import functools

import jax
import jax.numpy as jnp
import numpy as np
from jax import lax
from jax.experimental import pallas as pl
from jax.experimental.pallas import tpu as pltpu
from jax.sharding import PartitionSpec as P


QUERY_HEADS = 16
KEY_VALUE_HEADS = 8
HEAD_WIDTH = 128

EPS = 1e-05
ROPE_BASE = 500000.0
MASKED = -1e30
LANES = 128
AXES = ("seq", "section", "tp")


def rope_tables(positions, head_size):
    half_width = head_size // 2
    inverse_freq = ROPE_BASE ** (-jnp.arange(half_width).astype(jnp.float32) * (2.0 / head_size))
    angles = positions.astype(jnp.float32)[:, None] * inverse_freq[None, :]
    return (jnp.cos(angles), jnp.sin(angles))


def full_rope_tables(count, head_size):
    half_width = head_size // 2
    exponents = -np.arange(half_width).astype(np.float32) * np.float32(2.0 / head_size)
    inverse_freq = np.float32(ROPE_BASE) ** exponents
    angles = np.arange(count).astype(np.float32)[:, None] * inverse_freq[None, :]
    cosine, sine = np.cos(angles), np.sin(angles)
    return (
        np.concatenate([cosine, cosine], axis=1).astype(np.float32),
        np.concatenate([-sine, sine], axis=1).astype(np.float32),
    )


VMEM = pl.BlockSpec(memory_space=pltpu.VMEM)
SMEM = pl.BlockSpec(memory_space=pltpu.SMEM)
ANY = pl.BlockSpec(memory_space=pl.ANY)
HBM = pl.BlockSpec(memory_space=pltpu.HBM)


def on_section(kernel, section):
    def gated(*refs):
        pl.when(lax.axis_index("section") == section)(lambda: kernel(*refs))

    return gated


def lookup_kernel(ids_smem, ids_row, table, out, strips, onehot, sems):
    @pl.when(lax.axis_index("section") > 0)
    def _():
        read_columns(ids_smem, ids_row, table, out, strips, onehot, sems)


def read_columns(ids_smem, ids_row, table, out, strips, onehot, sems):
    features, _ = table.shape
    count = ids_row.shape[1]

    def start(i, _):
        first = pl.multiple_of((ids_smem[i] // LANES) * LANES, LANES)
        pltpu.make_async_copy(
            table.at[:, pl.ds(first, LANES)],
            strips.at[:, pl.ds(pl.multiple_of(i * LANES, LANES), LANES)],
            sems.at[i],
        ).start()
        return 0

    lax.fori_loop(0, count, start, 0)
    lanes = lax.rem(ids_row[...], LANES)
    group = 8
    acc = jnp.zeros((features, count), jnp.float32)
    wide = group * LANES
    rows = lax.broadcasted_iota(jnp.int32, (wide, count), 0)
    target = lax.broadcasted_iota(jnp.int32, (1, count), 1) * LANES + lanes
    for g in range(count // group):
        onehot[g] = jnp.where(rows + g * wide == target, 1.0, 0.0).astype(jnp.bfloat16)
    for g in range(count // group):
        for i in range(g * group, (g + 1) * group):
            pltpu.make_async_copy(
                table.at[:, pl.ds(0, LANES)],
                strips.at[:, pl.ds(i * LANES, LANES)],
                sems.at[i],
            ).wait()
        acc = acc + jnp.dot(
            strips[:, g * wide : (g + 1) * wide], onehot[g], preferred_element_type=jnp.float32
        )
    out[...] = acc.T.astype(jnp.bfloat16)


def lookup(ids, table):
    count, features = ids.shape[0], table.shape[0]
    return pl.pallas_call(
        lookup_kernel,
        out_shape=jax.ShapeDtypeStruct((count, features), jnp.bfloat16),
        in_specs=[SMEM, VMEM, ANY],
        out_specs=VMEM,
        scratch_shapes=[
            pltpu.VMEM((features, count * LANES), jnp.bfloat16),
            pltpu.VMEM((count // 8, 8 * LANES, count), jnp.bfloat16),
            pltpu.SemaphoreType.DMA((count,)),
        ],
        name="lookup",
        compiler_params=pltpu.CompilerParams(vmem_limit_bytes=16 << 20),
    )(ids, ids.reshape(1, count), table)


def send_order(ways):
    return sorted(range(ways), key=lambda k: -min(k, ways - k))


def whole_piece(rank, k, ways, parts):
    if len(parts) == 1:
        return parts[0][...]
    even = lax.rem(rank + ways - k, 2) == 0
    first, second = parts[0][...], parts[1][...]
    return jnp.concatenate([jnp.where(even, first, second), jnp.where(even, second, first)], axis=0)


def project_kernel(*refs, ways, split, last):
    pieces, (gain, weight, message, *kept) = refs[: ways * split], refs[ways * split :]
    rank, group = lax.axis_index("tp"), lax.axis_index("seq")
    width = pieces[0].shape[1]
    squares = None
    acc = None
    for n, k in enumerate(send_order(ways)):
        piece = whole_piece(rank, k, ways, pieces[n * split : (n + 1) * split])
        if last:
            kept[2][:, pl.ds(pl.multiple_of(lax.rem(rank + ways - k, ways) * width, width), width)] = piece
        elif k == 0:
            kept[0][...] = piece
        values = piece.astype(jnp.float32)
        square = jnp.sum(values * values, axis=1, keepdims=True)
        squares = square if squares is None else squares + square
        first = pl.multiple_of(lax.rem(rank + ways - k, ways) * width, width)
        scaled = (values * gain[:, pl.ds(first, width)]).astype(jnp.bfloat16)
        part = jnp.dot(scaled, weight[0, pl.ds(first, width), :], preferred_element_type=jnp.float32)
        acc = part if acc is None else acc + part
    cols = acc.shape[1]
    message[:, :cols] = acc.astype(jnp.bfloat16)
    high = squares.astype(jnp.bfloat16)
    low = squares - high.astype(jnp.float32)
    lane = lax.broadcasted_iota(jnp.int32, (acc.shape[0], LANES), 1)
    message[:, cols:] = jnp.where(lane < LANES // 2, high.astype(jnp.float32), low).astype(jnp.bfloat16)
    if last:
        mine, other, whole = kept
        block, quarter = mine.shape
        first = pl.multiple_of(lax.rem(rank, 2) * quarter, quarter)
        mine[...] = whole[pl.ds(pl.multiple_of(group * block, block), block), pl.ds(first, quarter)]
        other[...] = whole[pl.ds(pl.multiple_of((1 - group) * block, block), block), pl.ds(first, quarter)]


def project(section, pieces, gain, weight, ways, last):
    split = len(pieces) // ways
    rows, width = pieces[0].shape[0] * split, pieces[0].shape[1]
    cols = weight.shape[2]
    kept = [(rows // 2, 2 * width)] * 2 if last else [(rows, width)]
    return pl.pallas_call(
        on_section(functools.partial(project_kernel, ways=ways, split=split, last=last), section),
        out_shape=[
            jax.ShapeDtypeStruct((rows, cols + LANES), jnp.bfloat16),
        ]
        + [jax.ShapeDtypeStruct(shape, jnp.bfloat16) for shape in kept],
        in_specs=[VMEM] * (len(pieces) + 2),
        out_specs=[VMEM] * (1 + len(kept)),
        scratch_shapes=[pltpu.VMEM((rows, ways * width), jnp.bfloat16)] if last else [],
        name="project",
        compiler_params=pltpu.CompilerParams(vmem_limit_bytes=6 << 20),
    )(*pieces, gain, weight)


def stage_kernel(weight, after, out, sem, *, section):
    def bring():
        copy = pltpu.make_async_copy(weight, out, sem)
        copy.start()
        copy.wait()

    if section is None:
        bring()
    else:
        pl.when(lax.axis_index("section") == section)(bring)


def stage(weight, after, section=None):
    return pl.pallas_call(
        functools.partial(stage_kernel, section=section),
        out_shape=jax.ShapeDtypeStruct(weight.shape, weight.dtype),
        in_specs=[ANY if section is None else HBM, ANY],
        out_specs=VMEM,
        scratch_shapes=[pltpu.SemaphoreType.DMA],
        name="stage",
        compiler_params=pltpu.CompilerParams(vmem_limit_bytes=1 << 20),
    )(weight, after)


def attended_heads(total, inverse, cosine, sine, block, query_heads, key_value_heads, only):
    rows = total.shape[0]
    asked = rows if only is None else block
    repeat = query_heads // key_value_heads

    def head(i):
        return total[:, i * HEAD_WIDTH : (i + 1) * HEAD_WIDTH] * inverse

    def chosen(values):
        if only is None:
            return values
        blocks = [values[i * block : (i + 1) * block] for i in range(rows // block)]
        picked = blocks[0]
        for i in range(1, len(blocks)):
            picked = jnp.where(only == i, blocks[i], picked)
        return picked

    def rotated(i, pick=lambda values: values):
        values = pick(head(i))
        turned = values * pick(cosine) + pltpu.roll(values, HEAD_WIDTH // 2, 1) * pick(sine)
        return turned.astype(jnp.bfloat16)

    row = lax.broadcasted_iota(jnp.int32, (asked, rows), 0)
    row = row if only is None else row + only * block
    col = lax.broadcasted_iota(jnp.int32, (asked, rows), 1)
    row_block, col_block = row // block, col // block
    allowed = ((row_block == col_block) & (col <= row)) | ((col_block == 0) & (row_block > 0))
    keys = [rotated(query_heads + j) for j in range(key_value_heads)]
    held = [head(query_heads + key_value_heads + j).astype(jnp.bfloat16) for j in range(key_value_heads)]
    results = []
    for i in range(query_heads):
        scores = lax.dot_general(
            rotated(i, chosen), keys[i // repeat], (((1,), (1,)), ((), ())), preferred_element_type=jnp.float32
        ) * HEAD_WIDTH ** (-0.5)
        scores = jnp.where(allowed, scores, MASKED)
        top = jnp.max(scores, axis=1, keepdims=True)
        powers = jnp.exp(scores - top)
        weights = (powers / jnp.sum(powers, axis=1, keepdims=True)).astype(jnp.bfloat16)
        results.append(
            jnp.dot(weights, held[i // repeat], preferred_element_type=jnp.float32).astype(jnp.bfloat16)
        )
    return jnp.concatenate(results, axis=1)


def summed(got, mine, features):
    cols = mine.shape[1] - LANES
    squares = sum(
        message[:, at : at + 1].astype(jnp.float32) for message in (got, mine) for at in (cols, cols + LANES // 2)
    )
    inverse = lax.rsqrt(squares / features + EPS)
    return mine[:, :cols].astype(jnp.float32) + got[:, :cols].astype(jnp.float32), inverse


def times_transposed(left, right):
    return lax.dot_general(left, right, (((1,), (1,)), ((), ())), preferred_element_type=jnp.float32)


def attend_kernel(got, mine, cosine, sine, lent, *refs, ways, block, features, heads):
    outs, (weight, sem) = refs[:ways], refs[ways:]
    copy = pltpu.make_async_copy(lent, weight, sem)
    copy.start()
    rank = lax.axis_index("tp")
    width = weight.shape[1] // ways
    total, inverse = summed(got, mine, features)
    attended = attended_heads(total, inverse, cosine[...], sine[...], block, *heads, None)
    copy.wait()
    for k in range(ways):
        first = pl.multiple_of(lax.rem(rank + k, ways) * width, width)
        outs[k][...] = times_transposed(attended, weight[0, pl.ds(first, width), :]).astype(outs[k].dtype)


def last_kernel(got, mine, cosine, sine, lent, far_weight, *refs, ways, block, features, heads):
    outs, (weight, sem, other_weight, other_sem, slots) = refs[:ways], refs[ways:]
    rank, group = lax.axis_index("tp"), lax.axis_index("seq")
    width = outs[0].shape[1]
    copies = [
        pltpu.make_async_copy(lent, weight, sem),
        pltpu.make_async_copy(far_weight, other_weight, other_sem),
    ]
    for copy in copies:
        copy.start()
    total, inverse = summed(got, mine, features)
    attended = attended_heads(total, inverse, cosine[...], sine[...], block, *heads, group)
    per_half = weight.shape[1] // width
    for side, held, copy in ((group, weight, copies[0]), (1 - group, other_weight, copies[1])):
        copy.wait()
        for i in range(per_half):
            shift = lax.rem(side * per_half + i + ways - rank, ways)
            product = times_transposed(attended, held[0, i * width : (i + 1) * width, :])
            slots[shift] = product.astype(slots.dtype)
    for k in range(ways):
        outs[k][...] = slots[k]


def attend(section, got, mine, cosine, sine, weights, ways, block, features, heads):
    last = len(weights) > 1
    shape = (block, features // ways) if last else (mine.shape[0], weights[0].shape[1] // ways)
    return pl.pallas_call(
        on_section(
            functools.partial(
                last_kernel if last else attend_kernel, ways=ways, block=block, features=features, heads=heads
            ),
            section,
        ),
        out_shape=[jax.ShapeDtypeStruct(shape, jnp.bfloat16) for _ in range(ways)],
        in_specs=[VMEM] * 4 + [HBM] * len(weights),
        out_specs=[VMEM] * ways,
        scratch_shapes=[
            scratch
            for weight in weights
            for scratch in (pltpu.VMEM(weight.shape, jnp.bfloat16), pltpu.SemaphoreType.DMA)
        ]
        + ([pltpu.VMEM((ways,) + shape, jnp.bfloat16)] if last else []),
        name="attend",
        compiler_params=pltpu.CompilerParams(vmem_limit_bytes=8 << 20),
    )(got, mine, cosine, sine, *weights)


def combine_kernel(*refs, ways):
    parts, (residual, out) = refs[:ways], refs[ways:]
    total = parts[0][...].astype(jnp.float32)
    for part in parts[1:]:
        total = total + part[...].astype(jnp.float32)
    out[...] = (residual[...].astype(jnp.float32) + total).astype(jnp.bfloat16)


def combine(parts, residual):
    return pl.pallas_call(
        functools.partial(combine_kernel, ways=len(parts)),
        out_shape=jax.ShapeDtypeStruct(residual.shape, jnp.bfloat16),
        in_specs=[VMEM] * (len(parts) + 1),
        out_specs=VMEM,
        name="combine",
        compiler_params=pltpu.CompilerParams(vmem_limit_bytes=4 << 20),
    )(*parts, residual)


def finish_kernel(*refs, ways):
    parts, (residual, third, first, second, out) = refs[:ways], refs[ways:]
    group, section = lax.axis_index("seq"), lax.axis_index("section")
    sections = lax.axis_size("section")
    width = first.shape[1]

    @pl.when(section == sections - 1)
    def _():
        total = parts[0][...].astype(jnp.float32)
        for part in parts[1:]:
            total = total + part[...].astype(jnp.float32)
        out[0] = (residual[...].astype(jnp.float32) + total).astype(jnp.bfloat16)

    @pl.when(section == sections - 2)
    def _():
        out[0] = third[...]

    @pl.when(section < sections - 2)
    def _():
        out[0, :, :width] = jnp.where(group == 0, first[...], second[...])
        out[0, :, width:] = jnp.where(group == 0, second[...], first[...])


def finish(parts, residual, third, earlier):
    return pl.pallas_call(
        functools.partial(finish_kernel, ways=len(parts)),
        out_shape=jax.ShapeDtypeStruct((1,) + residual.shape, jnp.bfloat16),
        in_specs=[VMEM] * (len(parts) + 4),
        out_specs=VMEM,
        name="finish",
        compiler_params=pltpu.CompilerParams(vmem_limit_bytes=4 << 20),
    )(*parts, residual, third, *earlier)


def stationary_body(token_ids, embed_columns, norm_gain, qkv_weight, out_weight):
    seq_count = lax.axis_size("seq")
    sections = lax.axis_size("section")
    ways = lax.axis_size("tp")
    s, c, t = lax.axis_index("seq"), lax.axis_index("section"), lax.axis_index("tp")
    block = token_ids.shape[0]
    rows = block * seq_count
    width = embed_columns.shape[0]
    half = qkv_weight.shape[1]
    features = half * seq_count
    heads = (QUERY_HEADS // ways, KEY_VALUE_HEADS // ways)

    def at(seq, section, tp):
        return (seq * sections + section) * ways + tp

    def moved(value, pairs):
        return lax.ppermute(value, AXES, pairs)

    gain = lax.dynamic_slice_in_dim(norm_gain, s * half, half, axis=1).astype(jnp.float32)
    cosine, sine = (jnp.asarray(table) for table in full_rope_tables(rows, HEAD_WIDTH))

    def partner(section):
        return section ^ 1

    everywhere = [(s1, t1) for s1 in range(seq_count) for t1 in range(ways)]

    lent = lax.ppermute(out_weight, "section", [(i, partner(i)) for i in range(sections)])
    end = sections - 1
    lent_far = moved(out_weight, [(at(s1, end, t1), at(1 - s1, partner(end), t1)) for s1, t1 in everywhere])

    other_ids = lax.ppermute(token_ids, "seq", [(0, 1), (1, 0)])
    servers = {0: lambda t1: 1, 1: lambda t1: 2 + t1 // 2}
    ids = jnp.where(c == 1, token_ids, other_ids)
    looked = lookup(ids, embed_columns)
    arrivals = {}
    for group in range(2):
        for k in send_order(ways):
            pairs = []
            for s1, t1 in everywhere:
                b = s1 * ways + (t1 - k) % ways
                pairs.append((at(b % seq_count, servers[group](t1), b // seq_count), at(s1, 0, t1)))
            arrivals[k, group] = moved(looked, pairs)
    staged = stage(qkv_weight, looked)
    pieces = [arrivals[k, group] for k in send_order(ways) for group in range(2)]

    def shifted(source, target, k):
        if k == 0 and partner(source) == target:
            return [(at(s1, i, t1), at(s1, partner(i), t1)) for i in range(source % 2, sections, 2) for s1, t1 in everywhere]
        return [(at(s1, source, t1), at(s1, target, (t1 + k) % ways)) for s1, t1 in everywhere]

    def crossed(source):
        return [
            (at(s1, i, t1), at(1 - s1, partner(i), t1))
            for i in (range(0, sections, 2) if source % 2 == 0 else [source])
            for s1, t1 in everywhere
        ]

    state = jnp.zeros((rows, width), jnp.bfloat16)
    earlier = []
    for layer in range(sections):
        aside = partner(layer)
        message, *kept = project(layer, pieces, gain, staged, ways, layer == end)
        if layer == end - 1:
            state, _ = lax.optimization_barrier((state, message))
            for m in range(2):
                chosen = lax.dynamic_slice_in_dim(state, lax.rem(t + m, 2) * block, block, axis=0)
                pairs = []
                for section in range(end - 1):
                    for s2, t2 in everywhere:
                        pairs.append((at(s2, section, t2), at((t2 + m) % 2, section, 2 * s2 + t2 // 2)))
                earlier.append(moved(chosen, pairs))
        got_far = moved(message, crossed(layer))
        got_near = moved(message, shifted(layer, aside, 0))
        if layer == end:
            break
        outs = attend(aside, got_far, got_near, cosine, sine, [lent], ways, block, features, heads)
        parts = [moved(outs[k], shifted(aside, layer, k)) for k in send_order(ways)]
        fresh = combine(parts, kept[0])
        if layer == end - 1:
            staged = stage(qkv_weight, fresh, end)
        else:
            state = jnp.where(c == layer, fresh, state)
        pieces = [moved(fresh, shifted(layer, layer + 1, k)) for k in send_order(ways)]

    mine, other = kept
    brought = moved(other, [(at(t1 // 2, end, t1), at(1 - t1 // 2, end, t1)) for t1 in range(ways)])
    residual = jnp.where(s == t // 2, mine, brought)
    outs = attend(aside, got_far, got_near, cosine, sine, [lent, lent_far], ways, block, features, heads)
    parts = [moved(outs[k], shifted(partner(end), end, k)) for k in send_order(ways)]
    third = moved(residual, shifted(end, partner(end), 0))
    return finish(parts, residual, third, earlier)


def passed_along(value, axis, steps):
    count = lax.axis_size(axis)
    leading, last = (max(0, -steps), min(count, count - steps))
    return lax.ppermute(value, axis, [(source, source + steps) for source in range(leading, last)])


def from_root(value, axis, root):
    mine = lax.axis_index(axis) == root
    return lax.psum(jnp.where(mine, value, jnp.zeros_like(value)), axis)


def rotate_half(heads, cosine_table, sine_values):
    half_width = heads.shape[-1] // 2
    first_half = heads[..., :half_width]
    second = heads[..., half_width:]
    cosine_table = cosine_table[:, None, :]
    sine_values = sine_values[:, None, :]
    return jnp.concatenate(
        [
            first_half * cosine_table - second * sine_values,
            second * cosine_table + first_half * sine_values,
        ],
        axis=-1,
    )


def norm_rows(row_block, gain_row):
    values = row_block.astype(jnp.float32)
    inverse_rms = lax.rsqrt(jnp.mean(values * values, axis=-1, keepdims=True) + EPS)
    return (values * inverse_rms * gain_row[None, :]).astype(jnp.bfloat16)


def gathered_project(full_rows, gain_row, qkv_full, positions, query_heads, key_value_heads):
    row_count = full_rows.shape[0]
    normed = norm_rows(full_rows, gain_row)
    projected_rows = jnp.dot(normed, qkv_full, preferred_element_type=jnp.float32)
    projected_rows = projected_rows.reshape(row_count, query_heads + 2 * key_value_heads, HEAD_WIDTH)
    cosine_table, sine_values = rope_tables(positions, HEAD_WIDTH)
    query_rows = rotate_half(projected_rows[:, :query_heads], cosine_table, sine_values)
    key_head_rows = rotate_half(
        projected_rows[:, query_heads : query_heads + key_value_heads], cosine_table, sine_values
    )
    value_head_rows = projected_rows[:, query_heads + key_value_heads :]
    return tuple(v.astype(jnp.bfloat16) for v in (query_rows, key_head_rows, value_head_rows))


def gathered_attend(query_rows, key_head_rows, value_head_rows, allowed):
    row_count, query_heads, head_size = query_rows.shape
    key_value_heads = key_head_rows.shape[1]
    query_groups = query_rows.reshape(row_count, key_value_heads, query_heads // key_value_heads, head_size)
    scores = jnp.einsum(
        "rkph,ckh->kprc", query_groups, key_head_rows, preferred_element_type=jnp.float32
    ) * head_size ** (-0.5)
    scores = jnp.where(allowed[None, None], scores, MASKED)
    weights = jax.nn.softmax(scores, axis=-1).astype(jnp.bfloat16)
    attended = jnp.einsum("kprc,ckh->rkph", weights, value_head_rows, preferred_element_type=jnp.float32)
    return attended.reshape(row_count, query_heads * head_size).astype(jnp.bfloat16)


def gathered_combine(current, attended, out_full):
    partial_value = lax.dot_general(
        attended, out_full, (((1,), (1,)), ((), ())), preferred_element_type=jnp.float32
    )
    summed = lax.psum_scatter(
        partial_value.astype(jnp.bfloat16), "tp", scatter_dimension=1, tiled=True
    ).astype(jnp.float32)
    return (current.astype(jnp.float32) + summed).astype(jnp.bfloat16)


def gathered_body(token_ids, embed_columns, norm_gain, qkv_weight, out_weight):
    seq_count = lax.axis_size("seq")
    section_count = lax.axis_size("section")
    tensor_parallel_count = lax.axis_size("tp")
    group_index = lax.axis_index("seq")
    section_index = lax.axis_index("section")
    block_row_slice = token_ids.shape[0]
    feature_cols = embed_columns.shape[0] * seq_count
    query_heads = QUERY_HEADS // tensor_parallel_count
    key_value_heads = KEY_VALUE_HEADS // tensor_parallel_count
    every_id = lax.all_gather(token_ids, "seq", axis=0, tiled=True)
    looked = jnp.take(embed_columns, every_id, axis=1)
    current = lax.all_to_all(looked, "seq", split_axis=1, concat_axis=0, tiled=True).T
    qkv_full = lax.all_gather(qkv_weight, "seq", axis=1, tiled=True)[0]
    out_full = lax.all_gather(out_weight, "seq", axis=1, tiled=True)[0]
    gain_row = norm_gain[0].astype(jnp.float32)
    outputs = jnp.zeros((block_row_slice, feature_cols), jnp.bfloat16)
    row_ids = jnp.arange(block_row_slice)[:, None]
    column = jnp.arange(2 * block_row_slice)[None, :]
    positions = group_index * block_row_slice + jnp.arange(block_row_slice)
    allowed = jnp.where(column < block_row_slice, group_index > 0, column - block_row_slice <= row_ids)
    for step_number in range(section_count):
        full_rows = lax.all_gather(current, "tp", axis=1, tiled=True)
        query_rows, key_head_rows, value_head_rows = gathered_project(
            full_rows, gain_row, qkv_full, positions, query_heads, key_value_heads
        )
        anchor_heads = from_root(key_head_rows, "seq", 0)
        anchor_values = from_root(value_head_rows, "seq", 0)
        both_keys = jnp.concatenate([anchor_heads, key_head_rows], axis=0)
        both_values = jnp.concatenate([anchor_values, value_head_rows], axis=0)
        attended = gathered_attend(query_rows, both_keys, both_values, allowed)
        new_rows = gathered_combine(current, attended, out_full)
        outputs = jnp.where(section_index == step_number, new_rows, outputs)
        if step_number + 1 < section_count:
            current = passed_along(new_rows, "section", 1)
    return outputs[None]


def solution(mesh):
    placed = (
        P("seq"),
        P(("tp", "seq"), None),
        P("section", None),
        P("section", "seq", "tp"),
        P("section", "seq", "tp"),
    )
    sizes = mesh.shape
    small = sizes["seq"] == 2 and sizes["tp"] == 4 and sizes["section"] == 4
    return jax.shard_map(
        stationary_body if small else gathered_body,
        mesh=mesh,
        in_specs=placed,
        out_specs=P("section", "seq", "tp"),
        check_vma=False,
    )
```

```python
import functools

import jax
import jax.numpy as jnp
import numpy as np
from jax import lax
from jax.experimental import pallas as pl
from jax.experimental.pallas import tpu as pltpu
from jax.sharding import PartitionSpec as P


QUERY_HEADS = 16
KEY_VALUE_HEADS = 8
HEAD_WIDTH = 128

EPS = 1e-05
ROPE_BASE = 500000.0
MASKED = -1e30
LANES = 128
AXES = ("seq", "section", "tp")


def rope_tables(positions, head_size):
    half_width = head_size // 2
    inverse_freq = ROPE_BASE ** (-jnp.arange(half_width).astype(jnp.float32) * (2.0 / head_size))
    angles = positions.astype(jnp.float32)[:, None] * inverse_freq[None, :]
    return (jnp.cos(angles), jnp.sin(angles))


def full_rope_tables(count, head_size):
    half_width = head_size // 2
    exponents = -np.arange(half_width).astype(np.float32) * np.float32(2.0 / head_size)
    inverse_freq = np.float32(ROPE_BASE) ** exponents
    angles = np.arange(count).astype(np.float32)[:, None] * inverse_freq[None, :]
    cosine, sine = np.cos(angles), np.sin(angles)
    return (
        np.concatenate([cosine, cosine], axis=1).astype(np.float32),
        np.concatenate([-sine, sine], axis=1).astype(np.float32),
    )


VMEM = pl.BlockSpec(memory_space=pltpu.VMEM)
SMEM = pl.BlockSpec(memory_space=pltpu.SMEM)
ANY = pl.BlockSpec(memory_space=pl.ANY)
HBM = pl.BlockSpec(memory_space=pltpu.HBM)


def on_section(kernel, section):
    def gated(*refs):
        pl.when(lax.axis_index("section") == section)(lambda: kernel(*refs))

    return gated


def lookup_kernel(ids_smem, ids_row, table, out, strips, onehot, sems):
    @pl.when(lax.axis_index("section") > 0)
    def _():
        read_columns(ids_smem, ids_row, table, out, strips, onehot, sems)


def read_columns(ids_smem, ids_row, table, out, strips, onehot, sems):
    features, _ = table.shape
    count = ids_row.shape[1]

    def start(i, _):
        first = pl.multiple_of((ids_smem[i] // LANES) * LANES, LANES)
        pltpu.make_async_copy(
            table.at[:, pl.ds(first, LANES)],
            strips.at[:, pl.ds(pl.multiple_of(i * LANES, LANES), LANES)],
            sems.at[i],
        ).start()
        return 0

    lax.fori_loop(0, count, start, 0)
    lanes = lax.rem(ids_row[...], LANES)
    group = 8
    acc = jnp.zeros((features, count), jnp.float32)
    wide = group * LANES
    rows = lax.broadcasted_iota(jnp.int32, (wide, count), 0)
    target = lax.broadcasted_iota(jnp.int32, (1, count), 1) * LANES + lanes
    for g in range(count // group):
        onehot[g] = jnp.where(rows + g * wide == target, 1.0, 0.0).astype(jnp.bfloat16)
    for g in range(count // group):
        for i in range(g * group, (g + 1) * group):
            pltpu.make_async_copy(
                table.at[:, pl.ds(0, LANES)],
                strips.at[:, pl.ds(i * LANES, LANES)],
                sems.at[i],
            ).wait()
        acc = acc + jnp.dot(
            strips[:, g * wide : (g + 1) * wide], onehot[g], preferred_element_type=jnp.float32
        )
    out[...] = acc.T.astype(jnp.bfloat16)


def lookup(ids, table):
    count, features = ids.shape[0], table.shape[0]
    return pl.pallas_call(
        lookup_kernel,
        out_shape=jax.ShapeDtypeStruct((count, features), jnp.bfloat16),
        in_specs=[SMEM, VMEM, ANY],
        out_specs=VMEM,
        scratch_shapes=[
            pltpu.VMEM((features, count * LANES), jnp.bfloat16),
            pltpu.VMEM((count // 8, 8 * LANES, count), jnp.bfloat16),
            pltpu.SemaphoreType.DMA((count,)),
        ],
        name="lookup",
        compiler_params=pltpu.CompilerParams(vmem_limit_bytes=16 << 20),
    )(ids, ids.reshape(1, count), table)


def send_order(ways):
    return sorted(range(ways), key=lambda k: -min(k, ways - k))


def whole_piece(rank, k, ways, parts):
    if len(parts) == 1:
        return parts[0][...]
    even = lax.rem(rank + ways - k, 2) == 0
    first, second = parts[0][...], parts[1][...]
    return jnp.concatenate([jnp.where(even, first, second), jnp.where(even, second, first)], axis=0)


def project_kernel(*refs, ways, split, last):
    pieces, (gain, weight, message, *kept) = refs[: ways * split], refs[ways * split :]
    rank, group = lax.axis_index("tp"), lax.axis_index("seq")
    width = pieces[0].shape[1]
    squares = None
    acc = None
    for n, k in enumerate(send_order(ways)):
        piece = whole_piece(rank, k, ways, pieces[n * split : (n + 1) * split])
        if last:
            kept[2][:, pl.ds(pl.multiple_of(lax.rem(rank + ways - k, ways) * width, width), width)] = piece
        elif k == 0:
            kept[0][...] = piece
        values = piece.astype(jnp.float32)
        square = jnp.sum(values * values, axis=1, keepdims=True)
        squares = square if squares is None else squares + square
        first = pl.multiple_of(lax.rem(rank + ways - k, ways) * width, width)
        scaled = (values * gain[:, pl.ds(first, width)]).astype(jnp.bfloat16)
        part = jnp.dot(scaled, weight[0, pl.ds(first, width), :], preferred_element_type=jnp.float32)
        acc = part if acc is None else acc + part
    cols = acc.shape[1]
    message[:, :cols] = acc.astype(jnp.bfloat16)
    high = squares.astype(jnp.bfloat16)
    low = squares - high.astype(jnp.float32)
    lane = lax.broadcasted_iota(jnp.int32, (acc.shape[0], LANES), 1)
    message[:, cols:] = jnp.where(lane < LANES // 2, high.astype(jnp.float32), low).astype(jnp.bfloat16)
    if last:
        mine, other, whole = kept
        block, quarter = mine.shape
        first = pl.multiple_of(lax.rem(rank, 2) * quarter, quarter)
        mine[...] = whole[pl.ds(pl.multiple_of(group * block, block), block), pl.ds(first, quarter)]
        other[...] = whole[pl.ds(pl.multiple_of((1 - group) * block, block), block), pl.ds(first, quarter)]


def project(section, pieces, gain, weight, ways, last):
    split = len(pieces) // ways
    rows, width = pieces[0].shape[0] * split, pieces[0].shape[1]
    cols = weight.shape[2]
    kept = [(rows // 2, 2 * width)] * 2 if last else [(rows, width)]
    return pl.pallas_call(
        on_section(functools.partial(project_kernel, ways=ways, split=split, last=last), section),
        out_shape=[
            jax.ShapeDtypeStruct((rows, cols + LANES), jnp.bfloat16),
        ]
        + [jax.ShapeDtypeStruct(shape, jnp.bfloat16) for shape in kept],
        in_specs=[VMEM] * (len(pieces) + 2),
        out_specs=[VMEM] * (1 + len(kept)),
        scratch_shapes=[pltpu.VMEM((rows, ways * width), jnp.bfloat16)] if last else [],
        name="project",
        compiler_params=pltpu.CompilerParams(vmem_limit_bytes=6 << 20),
    )(*pieces, gain, weight)


def stage_kernel(weight, after, out, sem):
    copy = pltpu.make_async_copy(weight, out, sem)
    copy.start()
    copy.wait()


def stage(section, weight, after):
    return pl.pallas_call(
        on_section(stage_kernel, section),
        out_shape=jax.ShapeDtypeStruct(weight.shape, weight.dtype),
        in_specs=[HBM, ANY],
        out_specs=VMEM,
        scratch_shapes=[pltpu.SemaphoreType.DMA],
        name="stage",
        compiler_params=pltpu.CompilerParams(vmem_limit_bytes=1 << 20),
    )(weight, after)


def attended_heads(total, inverse, cosine, sine, block, query_heads, key_value_heads, only):
    rows = total.shape[0]
    asked = rows if only is None else block
    repeat = query_heads // key_value_heads

    def head(i):
        return total[:, i * HEAD_WIDTH : (i + 1) * HEAD_WIDTH] * inverse

    def chosen(values):
        if only is None:
            return values
        blocks = [values[i * block : (i + 1) * block] for i in range(rows // block)]
        picked = blocks[0]
        for i in range(1, len(blocks)):
            picked = jnp.where(only == i, blocks[i], picked)
        return picked

    def rotated(i, pick=lambda values: values):
        values = pick(head(i))
        turned = values * pick(cosine) + pltpu.roll(values, HEAD_WIDTH // 2, 1) * pick(sine)
        return turned.astype(jnp.bfloat16)

    row = lax.broadcasted_iota(jnp.int32, (asked, rows), 0)
    row = row if only is None else row + only * block
    col = lax.broadcasted_iota(jnp.int32, (asked, rows), 1)
    row_block, col_block = row // block, col // block
    allowed = ((row_block == col_block) & (col <= row)) | ((col_block == 0) & (row_block > 0))
    keys = [rotated(query_heads + j) for j in range(key_value_heads)]
    held = [head(query_heads + key_value_heads + j).astype(jnp.bfloat16) for j in range(key_value_heads)]
    queries = [rotated(i, chosen) for i in range(query_heads)]
    scores = [times_transposed(query, keys[i // repeat]) * HEAD_WIDTH ** (-0.5) for i, query in enumerate(queries)]
    scores = [jnp.where(allowed, score, MASKED) for score in scores]
    tops = [jnp.max(score, axis=1, keepdims=True) for score in scores]
    powers = [jnp.exp(score - top) for score, top in zip(scores, tops)]
    sums = [jnp.sum(power, axis=1, keepdims=True) for power in powers]
    weights = [(power / total_power).astype(jnp.bfloat16) for power, total_power in zip(powers, sums)]
    results = [
        jnp.dot(weight, held[i // repeat], preferred_element_type=jnp.float32).astype(jnp.bfloat16)
        for i, weight in enumerate(weights)
    ]
    return jnp.concatenate(results, axis=1)


def summed(got, mine, features):
    cols = mine.shape[1] - LANES
    squares = sum(
        message[:, at : at + 1].astype(jnp.float32) for message in (got, mine) for at in (cols, cols + LANES // 2)
    )
    inverse = lax.rsqrt(squares / features + EPS)
    return mine[:, :cols].astype(jnp.float32) + got[:, :cols].astype(jnp.float32), inverse


def times_transposed(left, right):
    return lax.dot_general(left, right, (((1,), (1,)), ((), ())), preferred_element_type=jnp.float32)


def attend_kernel(got, mine, cosine, sine, lent, *refs, ways, block, features, heads):
    outs, (weight, sem) = refs[:ways], refs[ways:]
    copy = pltpu.make_async_copy(lent, weight, sem)
    copy.start()
    rank = lax.axis_index("tp")
    width = weight.shape[1] // ways
    total, inverse = summed(got, mine, features)
    attended = attended_heads(total, inverse, cosine[...], sine[...], block, *heads, None)
    copy.wait()
    for k in range(ways):
        first = pl.multiple_of(lax.rem(rank + k, ways) * width, width)
        outs[k][...] = times_transposed(attended, weight[0, pl.ds(first, width), :]).astype(outs[k].dtype)


def last_kernel(got, mine, cosine, sine, lent, far_weight, *refs, ways, block, features, heads):
    outs, (weight, sem, other_weight, other_sem, slots) = refs[:ways], refs[ways:]
    rank, group = lax.axis_index("tp"), lax.axis_index("seq")
    width = outs[0].shape[1]
    copies = [
        pltpu.make_async_copy(lent, weight, sem),
        pltpu.make_async_copy(far_weight, other_weight, other_sem),
    ]
    for copy in copies:
        copy.start()
    total, inverse = summed(got, mine, features)
    attended = attended_heads(total, inverse, cosine[...], sine[...], block, *heads, group)
    per_half = weight.shape[1] // width
    for side, held, copy in ((group, weight, copies[0]), (1 - group, other_weight, copies[1])):
        copy.wait()
        for i in range(per_half):
            shift = lax.rem(side * per_half + i + ways - rank, ways)
            product = times_transposed(attended, held[0, i * width : (i + 1) * width, :])
            slots[shift] = product.astype(slots.dtype)
    for k in range(ways):
        outs[k][...] = slots[k]


def attend(section, got, mine, cosine, sine, weights, ways, block, features, heads):
    last = len(weights) > 1
    shape = (block, features // ways) if last else (mine.shape[0], weights[0].shape[1] // ways)
    return pl.pallas_call(
        on_section(
            functools.partial(
                last_kernel if last else attend_kernel, ways=ways, block=block, features=features, heads=heads
            ),
            section,
        ),
        out_shape=[jax.ShapeDtypeStruct(shape, jnp.bfloat16) for _ in range(ways)],
        in_specs=[VMEM] * 4 + [HBM] * len(weights),
        out_specs=[VMEM] * ways,
        scratch_shapes=[
            scratch
            for weight in weights
            for scratch in (pltpu.VMEM(weight.shape, jnp.bfloat16), pltpu.SemaphoreType.DMA)
        ]
        + ([pltpu.VMEM((ways,) + shape, jnp.bfloat16)] if last else []),
        name="attend",
        compiler_params=pltpu.CompilerParams(vmem_limit_bytes=8 << 20),
    )(got, mine, cosine, sine, *weights)


def combine_kernel(*refs, ways):
    parts, (residual, out) = refs[:ways], refs[ways:]
    total = parts[0][...].astype(jnp.float32)
    for part in parts[1:]:
        total = total + part[...].astype(jnp.float32)
    out[...] = (residual[...].astype(jnp.float32) + total).astype(jnp.bfloat16)


def combine(parts, residual):
    return pl.pallas_call(
        functools.partial(combine_kernel, ways=len(parts)),
        out_shape=jax.ShapeDtypeStruct(residual.shape, jnp.bfloat16),
        in_specs=[VMEM] * (len(parts) + 1),
        out_specs=VMEM,
        name="combine",
        compiler_params=pltpu.CompilerParams(vmem_limit_bytes=4 << 20),
    )(*parts, residual)


def finish_kernel(*refs, ways):
    parts, (residual, third, first, second, out) = refs[:ways], refs[ways:]
    group, section = lax.axis_index("seq"), lax.axis_index("section")
    sections = lax.axis_size("section")
    width = first.shape[1]

    @pl.when(section == sections - 1)
    def _():
        total = parts[0][...].astype(jnp.float32)
        for part in parts[1:]:
            total = total + part[...].astype(jnp.float32)
        out[0] = (residual[...].astype(jnp.float32) + total).astype(jnp.bfloat16)

    @pl.when(section == sections - 2)
    def _():
        out[0] = third[...]

    @pl.when(section < sections - 2)
    def _():
        out[0, :, :width] = jnp.where(group == 0, first[...], second[...])
        out[0, :, width:] = jnp.where(group == 0, second[...], first[...])


def finish(parts, residual, third, earlier):
    return pl.pallas_call(
        functools.partial(finish_kernel, ways=len(parts)),
        out_shape=jax.ShapeDtypeStruct((1,) + residual.shape, jnp.bfloat16),
        in_specs=[VMEM] * (len(parts) + 4),
        out_specs=VMEM,
        name="finish",
        compiler_params=pltpu.CompilerParams(vmem_limit_bytes=4 << 20),
    )(*parts, residual, third, *earlier)


def stationary_body(token_ids, embed_columns, norm_gain, qkv_weight, out_weight):
    seq_count = lax.axis_size("seq")
    sections = lax.axis_size("section")
    ways = lax.axis_size("tp")
    s, c, t = lax.axis_index("seq"), lax.axis_index("section"), lax.axis_index("tp")
    block = token_ids.shape[0]
    rows = block * seq_count
    width = embed_columns.shape[0]
    half = qkv_weight.shape[1]
    features = half * seq_count
    heads = (QUERY_HEADS // ways, KEY_VALUE_HEADS // ways)

    def at(seq, section, tp):
        return (seq * sections + section) * ways + tp

    def moved(value, pairs):
        return lax.ppermute(value, AXES, pairs)

    gain = lax.dynamic_slice_in_dim(norm_gain, s * half, half, axis=1).astype(jnp.float32)
    cosine, sine = (jnp.asarray(table) for table in full_rope_tables(rows, HEAD_WIDTH))

    def partner(section):
        return section ^ 1

    everywhere = [(s1, t1) for s1 in range(seq_count) for t1 in range(ways)]

    lent = lax.ppermute(out_weight, "section", [(i, partner(i)) for i in range(sections)])
    end = sections - 1
    lent_far = moved(out_weight, [(at(s1, end, t1), at(1 - s1, partner(end), t1)) for s1, t1 in everywhere])

    other_ids = lax.ppermute(token_ids, "seq", [(0, 1), (1, 0)])
    servers = {0: lambda t1: 1, 1: lambda t1: 2 + t1 // 2}
    ids = jnp.where(c == 1, token_ids, other_ids)
    looked = lookup(ids, embed_columns)
    arrivals = {}
    for group in range(2):
        for k in send_order(ways):
            pairs = []
            for s1, t1 in everywhere:
                b = s1 * ways + (t1 - k) % ways
                pairs.append((at(b % seq_count, servers[group](t1), b // seq_count), at(s1, 0, t1)))
            arrivals[k, group] = moved(looked, pairs)
    staged = stage(0, qkv_weight, looked)
    pieces = [arrivals[k, group] for k in send_order(ways) for group in range(2)]

    def shifted(source, target, k):
        if k == 0 and partner(source) == target:
            return [(at(s1, i, t1), at(s1, partner(i), t1)) for i in range(source % 2, sections, 2) for s1, t1 in everywhere]
        return [(at(s1, source, t1), at(s1, target, (t1 + k) % ways)) for s1, t1 in everywhere]

    def crossed(source):
        return [
            (at(s1, i, t1), at(1 - s1, partner(i), t1))
            for i in (range(0, sections, 2) if source % 2 == 0 else [source])
            for s1, t1 in everywhere
        ]

    state = jnp.zeros((rows, width), jnp.bfloat16)
    earlier = []
    for layer in range(sections):
        aside = partner(layer)
        message, *kept = project(layer, pieces, gain, staged, ways, layer == end)
        if layer == end - 1:
            state, _ = lax.optimization_barrier((state, message))
            for m in range(2):
                chosen = lax.dynamic_slice_in_dim(state, lax.rem(t + m, 2) * block, block, axis=0)
                pairs = []
                for section in range(end - 1):
                    for s2, t2 in everywhere:
                        pairs.append((at(s2, section, t2), at((t2 + m) % 2, section, 2 * s2 + t2 // 2)))
                earlier.append(moved(chosen, pairs))
        got_far = moved(message, crossed(layer))
        got_near = moved(message, shifted(layer, aside, 0))
        if layer == end:
            break
        outs = attend(aside, got_far, got_near, cosine, sine, [lent], ways, block, features, heads)
        parts = [moved(outs[k], shifted(aside, layer, k)) for k in send_order(ways)]
        fresh = combine(parts, kept[0])
        staged = stage(layer + 1, qkv_weight, fresh)
        if layer < end - 1:
            state = jnp.where(c == layer, fresh, state)
        pieces = [moved(fresh, shifted(layer, layer + 1, k)) for k in send_order(ways)]

    mine, other = kept
    brought = moved(other, [(at(t1 // 2, end, t1), at(1 - t1 // 2, end, t1)) for t1 in range(ways)])
    residual = jnp.where(s == t // 2, mine, brought)
    outs = attend(aside, got_far, got_near, cosine, sine, [lent, lent_far], ways, block, features, heads)
    parts = []
    for k in send_order(ways):
        parts.append(moved(outs[k], shifted(partner(end), end, k)))
    third = moved(residual, shifted(end, partner(end), 0))
    return finish(parts, residual, third, earlier)


def passed_along(value, axis, steps):
    count = lax.axis_size(axis)
    leading, last = (max(0, -steps), min(count, count - steps))
    return lax.ppermute(value, axis, [(source, source + steps) for source in range(leading, last)])


def from_root(value, axis, root):
    mine = lax.axis_index(axis) == root
    return lax.psum(jnp.where(mine, value, jnp.zeros_like(value)), axis)


def rotate_half(heads, cosine_table, sine_values):
    half_width = heads.shape[-1] // 2
    first_half = heads[..., :half_width]
    second = heads[..., half_width:]
    cosine_table = cosine_table[:, None, :]
    sine_values = sine_values[:, None, :]
    return jnp.concatenate(
        [
            first_half * cosine_table - second * sine_values,
            second * cosine_table + first_half * sine_values,
        ],
        axis=-1,
    )


def norm_rows(row_block, gain_row):
    values = row_block.astype(jnp.float32)
    inverse_rms = lax.rsqrt(jnp.mean(values * values, axis=-1, keepdims=True) + EPS)
    return (values * inverse_rms * gain_row[None, :]).astype(jnp.bfloat16)


def gathered_project(full_rows, gain_row, qkv_full, positions, query_heads, key_value_heads):
    row_count = full_rows.shape[0]
    normed = norm_rows(full_rows, gain_row)
    projected_rows = jnp.dot(normed, qkv_full, preferred_element_type=jnp.float32)
    projected_rows = projected_rows.reshape(row_count, query_heads + 2 * key_value_heads, HEAD_WIDTH)
    cosine_table, sine_values = rope_tables(positions, HEAD_WIDTH)
    query_rows = rotate_half(projected_rows[:, :query_heads], cosine_table, sine_values)
    key_head_rows = rotate_half(
        projected_rows[:, query_heads : query_heads + key_value_heads], cosine_table, sine_values
    )
    value_head_rows = projected_rows[:, query_heads + key_value_heads :]
    return tuple(v.astype(jnp.bfloat16) for v in (query_rows, key_head_rows, value_head_rows))


def gathered_attend(query_rows, key_head_rows, value_head_rows, allowed):
    row_count, query_heads, head_size = query_rows.shape
    key_value_heads = key_head_rows.shape[1]
    query_groups = query_rows.reshape(row_count, key_value_heads, query_heads // key_value_heads, head_size)
    scores = jnp.einsum(
        "rkph,ckh->kprc", query_groups, key_head_rows, preferred_element_type=jnp.float32
    ) * head_size ** (-0.5)
    scores = jnp.where(allowed[None, None], scores, MASKED)
    weights = jax.nn.softmax(scores, axis=-1).astype(jnp.bfloat16)
    attended = jnp.einsum("kprc,ckh->rkph", weights, value_head_rows, preferred_element_type=jnp.float32)
    return attended.reshape(row_count, query_heads * head_size).astype(jnp.bfloat16)


def gathered_combine(current, attended, out_full):
    partial_value = lax.dot_general(
        attended, out_full, (((1,), (1,)), ((), ())), preferred_element_type=jnp.float32
    )
    summed = lax.psum_scatter(
        partial_value.astype(jnp.bfloat16), "tp", scatter_dimension=1, tiled=True
    ).astype(jnp.float32)
    return (current.astype(jnp.float32) + summed).astype(jnp.bfloat16)


def gathered_body(token_ids, embed_columns, norm_gain, qkv_weight, out_weight):
    seq_count = lax.axis_size("seq")
    section_count = lax.axis_size("section")
    tensor_parallel_count = lax.axis_size("tp")
    group_index = lax.axis_index("seq")
    section_index = lax.axis_index("section")
    block_row_slice = token_ids.shape[0]
    feature_cols = embed_columns.shape[0] * seq_count
    query_heads = QUERY_HEADS // tensor_parallel_count
    key_value_heads = KEY_VALUE_HEADS // tensor_parallel_count
    every_id = lax.all_gather(token_ids, "seq", axis=0, tiled=True)
    looked = jnp.take(embed_columns, every_id, axis=1)
    current = lax.all_to_all(looked, "seq", split_axis=1, concat_axis=0, tiled=True).T
    qkv_full = lax.all_gather(qkv_weight, "seq", axis=1, tiled=True)[0]
    out_full = lax.all_gather(out_weight, "seq", axis=1, tiled=True)[0]
    gain_row = norm_gain[0].astype(jnp.float32)
    outputs = jnp.zeros((block_row_slice, feature_cols), jnp.bfloat16)
    row_ids = jnp.arange(block_row_slice)[:, None]
    column = jnp.arange(2 * block_row_slice)[None, :]
    positions = group_index * block_row_slice + jnp.arange(block_row_slice)
    allowed = jnp.where(column < block_row_slice, group_index > 0, column - block_row_slice <= row_ids)
    for step_number in range(section_count):
        full_rows = lax.all_gather(current, "tp", axis=1, tiled=True)
        query_rows, key_head_rows, value_head_rows = gathered_project(
            full_rows, gain_row, qkv_full, positions, query_heads, key_value_heads
        )
        anchor_heads = from_root(key_head_rows, "seq", 0)
        anchor_values = from_root(value_head_rows, "seq", 0)
        both_keys = jnp.concatenate([anchor_heads, key_head_rows], axis=0)
        both_values = jnp.concatenate([anchor_values, value_head_rows], axis=0)
        attended = gathered_attend(query_rows, both_keys, both_values, allowed)
        new_rows = gathered_combine(current, attended, out_full)
        outputs = jnp.where(section_index == step_number, new_rows, outputs)
        if step_number + 1 < section_count:
            current = passed_along(new_rows, "section", 1)
    return outputs[None]


def solution(mesh):
    placed = (
        P("seq"),
        P(("tp", "seq"), None),
        P("section", None),
        P("section", "seq", "tp"),
        P("section", "seq", "tp"),
    )
    sizes = mesh.shape
    small = sizes["seq"] == 2 and sizes["tp"] == 4 and sizes["section"] == 4
    return jax.shard_map(
        stationary_body if small else gathered_body,
        mesh=mesh,
        in_specs=placed,
        out_specs=P("section", "seq", "tp"),
        check_vma=False,
    )
```

```python
import functools

import jax
import jax.numpy as jnp
import numpy as np
from jax import lax
from jax.experimental import pallas as pl
from jax.experimental.pallas import tpu as pltpu
from jax.sharding import PartitionSpec as P


QUERY_HEADS = 16
KEY_VALUE_HEADS = 8
HEAD_WIDTH = 128

EPS = 1e-05
ROPE_BASE = 500000.0
MASKED = -1e30
LANES = 128
AXES = ("seq", "section", "tp")


def rope_tables(positions, head_size):
    half_width = head_size // 2
    inverse_freq = ROPE_BASE ** (-jnp.arange(half_width).astype(jnp.float32) * (2.0 / head_size))
    angles = positions.astype(jnp.float32)[:, None] * inverse_freq[None, :]
    return (jnp.cos(angles), jnp.sin(angles))


def full_rope_tables(count, head_size):
    half_width = head_size // 2
    exponents = -np.arange(half_width).astype(np.float32) * np.float32(2.0 / head_size)
    inverse_freq = np.float32(ROPE_BASE) ** exponents
    angles = np.arange(count).astype(np.float32)[:, None] * inverse_freq[None, :]
    cosine, sine = np.cos(angles), np.sin(angles)
    return (
        np.concatenate([cosine, cosine], axis=1).astype(np.float32),
        np.concatenate([-sine, sine], axis=1).astype(np.float32),
    )


VMEM = pl.BlockSpec(memory_space=pltpu.VMEM)
SMEM = pl.BlockSpec(memory_space=pltpu.SMEM)
ANY = pl.BlockSpec(memory_space=pl.ANY)
HBM = pl.BlockSpec(memory_space=pltpu.HBM)


def on_section(kernel, section):
    def gated(*refs):
        pl.when(lax.axis_index("section") == section)(lambda: kernel(*refs))

    return gated


def lookup_kernel(ids_smem, ids_row, table, out, strips, onehot, sems):
    @pl.when(lax.axis_index("section") > 0)
    def _():
        read_columns(ids_smem, ids_row, table, out, strips, onehot, sems)


def read_columns(ids_smem, ids_row, table, out, strips, onehot, sems):
    features, _ = table.shape
    count = ids_row.shape[1]

    def start(i, _):
        first = pl.multiple_of((ids_smem[i] // LANES) * LANES, LANES)
        pltpu.make_async_copy(
            table.at[:, pl.ds(first, LANES)],
            strips.at[:, pl.ds(pl.multiple_of(i * LANES, LANES), LANES)],
            sems.at[i],
        ).start()
        return 0

    lax.fori_loop(0, count, start, 0)
    lanes = lax.rem(ids_row[...], LANES)
    group = 8
    acc = jnp.zeros((features, count), jnp.float32)
    wide = group * LANES
    rows = lax.broadcasted_iota(jnp.int32, (wide, count), 0)
    target = lax.broadcasted_iota(jnp.int32, (1, count), 1) * LANES + lanes
    for g in range(count // group):
        onehot[g] = jnp.where(rows + g * wide == target, 1.0, 0.0).astype(jnp.bfloat16)
    for g in range(count // group):
        for i in range(g * group, (g + 1) * group):
            pltpu.make_async_copy(
                table.at[:, pl.ds(0, LANES)],
                strips.at[:, pl.ds(i * LANES, LANES)],
                sems.at[i],
            ).wait()
        acc = acc + jnp.dot(
            strips[:, g * wide : (g + 1) * wide], onehot[g], preferred_element_type=jnp.float32
        )
    out[...] = acc.T.astype(jnp.bfloat16)


def lookup(ids, table):
    count, features = ids.shape[0], table.shape[0]
    return pl.pallas_call(
        lookup_kernel,
        out_shape=jax.ShapeDtypeStruct((count, features), jnp.bfloat16),
        in_specs=[SMEM, VMEM, ANY],
        out_specs=VMEM,
        scratch_shapes=[
            pltpu.VMEM((features, count * LANES), jnp.bfloat16),
            pltpu.VMEM((count // 8, 8 * LANES, count), jnp.bfloat16),
            pltpu.SemaphoreType.DMA((count,)),
        ],
        name="lookup",
        compiler_params=pltpu.CompilerParams(vmem_limit_bytes=16 << 20),
    )(ids, ids.reshape(1, count), table)


def send_order(ways):
    return sorted(range(ways), key=lambda k: -min(k, ways - k))


def whole_piece(rank, k, ways, parts):
    if len(parts) == 1:
        return parts[0][...]
    even = lax.rem(rank + ways - k, 2) == 0
    first, second = parts[0][...], parts[1][...]
    return jnp.concatenate([jnp.where(even, first, second), jnp.where(even, second, first)], axis=0)


def project_kernel(*refs, ways, split, last):
    pieces, (gain, weight, message, *kept) = refs[: ways * split], refs[ways * split :]
    rank, group = lax.axis_index("tp"), lax.axis_index("seq")
    width = pieces[0].shape[1]
    squares = None
    acc = None
    for n, k in enumerate(send_order(ways)):
        piece = whole_piece(rank, k, ways, pieces[n * split : (n + 1) * split])
        if last:
            kept[2][:, pl.ds(pl.multiple_of(lax.rem(rank + ways - k, ways) * width, width), width)] = piece
        elif k == 0:
            kept[0][...] = piece
        values = piece.astype(jnp.float32)
        square = jnp.sum(values * values, axis=1, keepdims=True)
        squares = square if squares is None else squares + square
        first = pl.multiple_of(lax.rem(rank + ways - k, ways) * width, width)
        scaled = (values * gain[:, pl.ds(first, width)]).astype(jnp.bfloat16)
        part = jnp.dot(scaled, weight[0, pl.ds(first, width), :], preferred_element_type=jnp.float32)
        acc = part if acc is None else acc + part
    cols = acc.shape[1]
    message[:, :cols] = acc.astype(jnp.bfloat16)
    high = squares.astype(jnp.bfloat16)
    low = squares - high.astype(jnp.float32)
    lane = lax.broadcasted_iota(jnp.int32, (acc.shape[0], LANES), 1)
    message[:, cols:] = jnp.where(lane < LANES // 2, high.astype(jnp.float32), low).astype(jnp.bfloat16)
    if last:
        mine, other, whole = kept
        block, quarter = mine.shape
        first = pl.multiple_of(lax.rem(rank, 2) * quarter, quarter)
        mine[...] = whole[pl.ds(pl.multiple_of(group * block, block), block), pl.ds(first, quarter)]
        other[...] = whole[pl.ds(pl.multiple_of((1 - group) * block, block), block), pl.ds(first, quarter)]


def project(section, pieces, gain, weight, ways, last):
    split = len(pieces) // ways
    rows, width = pieces[0].shape[0] * split, pieces[0].shape[1]
    cols = weight.shape[2]
    kept = [(rows // 2, 2 * width)] * 2 if last else [(rows, width)]
    return pl.pallas_call(
        on_section(functools.partial(project_kernel, ways=ways, split=split, last=last), section),
        out_shape=[
            jax.ShapeDtypeStruct((rows, cols + LANES), jnp.bfloat16),
        ]
        + [jax.ShapeDtypeStruct(shape, jnp.bfloat16) for shape in kept],
        in_specs=[VMEM] * (len(pieces) + 2),
        out_specs=[VMEM] * (1 + len(kept)),
        scratch_shapes=[pltpu.VMEM((rows, ways * width), jnp.bfloat16)] if last else [],
        name="project",
        compiler_params=pltpu.CompilerParams(vmem_limit_bytes=6 << 20),
    )(*pieces, gain, weight)


def stage_kernel(weight, after, out, sem):
    copy = pltpu.make_async_copy(weight, out, sem)
    copy.start()
    copy.wait()


def stage(section, weight, after):
    return pl.pallas_call(
        on_section(stage_kernel, section),
        out_shape=jax.ShapeDtypeStruct(weight.shape, weight.dtype),
        in_specs=[HBM, ANY],
        out_specs=VMEM,
        scratch_shapes=[pltpu.SemaphoreType.DMA],
        name="stage",
        compiler_params=pltpu.CompilerParams(vmem_limit_bytes=1 << 20),
    )(weight, after)


def turn_kernel(weight, after, out, held, sem):
    copy = pltpu.make_async_copy(weight, held, sem)
    copy.start()
    copy.wait()
    out[...] = held[0].T


def turned(section, weight, after):
    return pl.pallas_call(
        on_section(turn_kernel, section),
        out_shape=jax.ShapeDtypeStruct(weight.shape[:0:-1], weight.dtype),
        in_specs=[HBM, ANY],
        out_specs=VMEM,
        scratch_shapes=[pltpu.VMEM(weight.shape, weight.dtype), pltpu.SemaphoreType.DMA],
        name="turn",
        compiler_params=pltpu.CompilerParams(vmem_limit_bytes=8 << 20),
    )(weight, after)


def attended_heads(total, inverse, cosine, sine, block, query_heads, key_value_heads, only):
    rows = total.shape[0]
    asked = rows if only is None else block
    repeat = query_heads // key_value_heads

    def head(i):
        return total[:, i * HEAD_WIDTH : (i + 1) * HEAD_WIDTH] * inverse

    def chosen(values):
        if only is None:
            return values
        blocks = [values[i * block : (i + 1) * block] for i in range(rows // block)]
        picked = blocks[0]
        for i in range(1, len(blocks)):
            picked = jnp.where(only == i, blocks[i], picked)
        return picked

    def rotated(i, pick=lambda values: values):
        values = pick(head(i))
        turned = values * pick(cosine) + pltpu.roll(values, HEAD_WIDTH // 2, 1) * pick(sine)
        return turned.astype(jnp.bfloat16)

    row = lax.broadcasted_iota(jnp.int32, (asked, rows), 0)
    row = row if only is None else row + only * block
    col = lax.broadcasted_iota(jnp.int32, (asked, rows), 1)
    row_block, col_block = row // block, col // block
    allowed = ((row_block == col_block) & (col <= row)) | ((col_block == 0) & (row_block > 0))
    keys = [rotated(query_heads + j) for j in range(key_value_heads)]
    held = [head(query_heads + key_value_heads + j).astype(jnp.bfloat16) for j in range(key_value_heads)]
    queries = [rotated(i, chosen) for i in range(query_heads)]
    scores = [times_transposed(query, keys[i // repeat]) * HEAD_WIDTH ** (-0.5) for i, query in enumerate(queries)]
    scores = [jnp.where(allowed, score, MASKED) for score in scores]
    tops = [jnp.max(score, axis=1, keepdims=True) for score in scores]
    powers = [jnp.exp(score - top) for score, top in zip(scores, tops)]
    sums = [jnp.sum(power, axis=1, keepdims=True) for power in powers]
    weights = [(power / total_power).astype(jnp.bfloat16) for power, total_power in zip(powers, sums)]
    results = [
        jnp.dot(weight, held[i // repeat], preferred_element_type=jnp.float32).astype(jnp.bfloat16)
        for i, weight in enumerate(weights)
    ]
    return jnp.concatenate(results, axis=1)


def summed(got, mine, features):
    cols = mine.shape[1] - LANES
    squares = sum(
        message[:, at : at + 1].astype(jnp.float32) for message in (got, mine) for at in (cols, cols + LANES // 2)
    )
    inverse = lax.rsqrt(squares / features + EPS)
    return mine[:, :cols].astype(jnp.float32) + got[:, :cols].astype(jnp.float32), inverse


def times_transposed(left, right):
    return lax.dot_general(left, right, (((1,), (1,)), ((), ())), preferred_element_type=jnp.float32)


def attend_kernel(got, mine, cosine, sine, weight, *outs, ways, block, features, heads):
    rank = lax.axis_index("tp")
    width = outs[0].shape[1]
    total, inverse = summed(got, mine, features)
    attended = attended_heads(total, inverse, cosine[...], sine[...], block, *heads, None)
    for k in range(ways):
        first = pl.multiple_of(lax.rem(rank + k, ways) * width, width)
        product = jnp.dot(attended, weight[:, pl.ds(first, width)], preferred_element_type=jnp.float32)
        outs[k][...] = product.astype(outs[k].dtype)


def last_kernel(got, mine, cosine, sine, weight, other_weight, *refs, ways, block, features, heads):
    outs, (slots,) = refs[:ways], refs[ways:]
    rank, group = lax.axis_index("tp"), lax.axis_index("seq")
    width = outs[0].shape[1]
    total, inverse = summed(got, mine, features)
    attended = attended_heads(total, inverse, cosine[...], sine[...], block, *heads, group)
    per_half = weight.shape[1] // width
    for side, held in ((group, weight), (1 - group, other_weight)):
        for i in range(per_half):
            shift = lax.rem(side * per_half + i + ways - rank, ways)
            columns = held[:, i * width : (i + 1) * width]
            slots[shift] = jnp.dot(attended, columns, preferred_element_type=jnp.float32).astype(slots.dtype)
    for k in range(ways):
        outs[k][...] = slots[k]


def attend(section, got, mine, cosine, sine, weights, ways, block, features, heads):
    last = len(weights) > 1
    shape = (block, features // ways) if last else (mine.shape[0], weights[0].shape[1] // ways)
    return pl.pallas_call(
        on_section(
            functools.partial(
                last_kernel if last else attend_kernel, ways=ways, block=block, features=features, heads=heads
            ),
            section,
        ),
        out_shape=[jax.ShapeDtypeStruct(shape, jnp.bfloat16) for _ in range(ways)],
        in_specs=[VMEM] * (4 + len(weights)),
        out_specs=[VMEM] * ways,
        scratch_shapes=[pltpu.VMEM((ways,) + shape, jnp.bfloat16)] if last else [],
        name="attend",
        compiler_params=pltpu.CompilerParams(vmem_limit_bytes=6 << 20),
    )(got, mine, cosine, sine, *weights)


def combine_kernel(*refs, ways):
    parts, (residual, out) = refs[:ways], refs[ways:]
    total = parts[0][...].astype(jnp.float32)
    for part in parts[1:]:
        total = total + part[...].astype(jnp.float32)
    out[...] = (residual[...].astype(jnp.float32) + total).astype(jnp.bfloat16)


def combine(parts, residual):
    return pl.pallas_call(
        functools.partial(combine_kernel, ways=len(parts)),
        out_shape=jax.ShapeDtypeStruct(residual.shape, jnp.bfloat16),
        in_specs=[VMEM] * (len(parts) + 1),
        out_specs=VMEM,
        name="combine",
        compiler_params=pltpu.CompilerParams(vmem_limit_bytes=4 << 20),
    )(*parts, residual)


def finish_kernel(*refs, ways):
    parts, (residual, third, first, second, out) = refs[:ways], refs[ways:]
    group, section = lax.axis_index("seq"), lax.axis_index("section")
    sections = lax.axis_size("section")
    width = first.shape[1]

    @pl.when(section == sections - 1)
    def _():
        total = parts[0][...].astype(jnp.float32)
        for part in parts[1:]:
            total = total + part[...].astype(jnp.float32)
        out[0] = (residual[...].astype(jnp.float32) + total).astype(jnp.bfloat16)

    @pl.when(section == sections - 2)
    def _():
        out[0] = third[...]

    @pl.when(section < sections - 2)
    def _():
        out[0, :, :width] = jnp.where(group == 0, first[...], second[...])
        out[0, :, width:] = jnp.where(group == 0, second[...], first[...])


def finish(parts, residual, third, earlier):
    return pl.pallas_call(
        functools.partial(finish_kernel, ways=len(parts)),
        out_shape=jax.ShapeDtypeStruct((1,) + residual.shape, jnp.bfloat16),
        in_specs=[VMEM] * (len(parts) + 4),
        out_specs=VMEM,
        name="finish",
        compiler_params=pltpu.CompilerParams(vmem_limit_bytes=4 << 20),
    )(*parts, residual, third, *earlier)


def stationary_body(token_ids, embed_columns, norm_gain, qkv_weight, out_weight):
    seq_count = lax.axis_size("seq")
    sections = lax.axis_size("section")
    ways = lax.axis_size("tp")
    s, c, t = lax.axis_index("seq"), lax.axis_index("section"), lax.axis_index("tp")
    block = token_ids.shape[0]
    rows = block * seq_count
    width = embed_columns.shape[0]
    half = qkv_weight.shape[1]
    features = half * seq_count
    heads = (QUERY_HEADS // ways, KEY_VALUE_HEADS // ways)

    def at(seq, section, tp):
        return (seq * sections + section) * ways + tp

    def moved(value, pairs):
        return lax.ppermute(value, AXES, pairs)

    gain = lax.dynamic_slice_in_dim(norm_gain, s * half, half, axis=1).astype(jnp.float32)
    cosine, sine = (jnp.asarray(table) for table in full_rope_tables(rows, HEAD_WIDTH))

    def partner(section):
        return section ^ 1

    everywhere = [(s1, t1) for s1 in range(seq_count) for t1 in range(ways)]

    lent = lax.ppermute(out_weight, "section", [(i, partner(i)) for i in range(sections)])
    end = sections - 1
    lent_far = moved(out_weight, [(at(s1, end, t1), at(1 - s1, partner(end), t1)) for s1, t1 in everywhere])

    other_ids = lax.ppermute(token_ids, "seq", [(0, 1), (1, 0)])
    servers = {0: lambda t1: 1, 1: lambda t1: 2 + t1 // 2}
    ids = jnp.where(c == 1, token_ids, other_ids)
    looked = lookup(ids, embed_columns)
    arrivals = {}
    for group in range(2):
        for k in send_order(ways):
            pairs = []
            for s1, t1 in everywhere:
                b = s1 * ways + (t1 - k) % ways
                pairs.append((at(b % seq_count, servers[group](t1), b // seq_count), at(s1, 0, t1)))
            arrivals[k, group] = moved(looked, pairs)
    staged = stage(0, qkv_weight, looked)
    out_turned = [turned(partner(0), lent, looked)]
    pieces = [arrivals[k, group] for k in send_order(ways) for group in range(2)]

    def shifted(source, target, k):
        if k == 0 and partner(source) == target:
            return [(at(s1, i, t1), at(s1, partner(i), t1)) for i in range(source % 2, sections, 2) for s1, t1 in everywhere]
        return [(at(s1, source, t1), at(s1, target, (t1 + k) % ways)) for s1, t1 in everywhere]

    def crossed(source):
        return [
            (at(s1, i, t1), at(1 - s1, partner(i), t1))
            for i in (range(0, sections, 2) if source % 2 == 0 else [source])
            for s1, t1 in everywhere
        ]

    state = jnp.zeros((rows, width), jnp.bfloat16)
    earlier = []
    for layer in range(sections):
        aside = partner(layer)
        message, *kept = project(layer, pieces, gain, staged, ways, layer == end)
        if layer == end - 1:
            state, _ = lax.optimization_barrier((state, message))
            for m in range(2):
                chosen = lax.dynamic_slice_in_dim(state, lax.rem(t + m, 2) * block, block, axis=0)
                pairs = []
                for section in range(end - 1):
                    for s2, t2 in everywhere:
                        pairs.append((at(s2, section, t2), at((t2 + m) % 2, section, 2 * s2 + t2 // 2)))
                earlier.append(moved(chosen, pairs))
        got_far = moved(message, crossed(layer))
        got_near = moved(message, shifted(layer, aside, 0))
        if layer == end:
            break
        outs = attend(aside, got_far, got_near, cosine, sine, out_turned, ways, block, features, heads)
        parts = [moved(outs[k], shifted(aside, layer, k)) for k in send_order(ways)]
        fresh = combine(parts, kept[0])
        staged = stage(layer + 1, qkv_weight, fresh)
        lenders = [lent, lent_far] if layer + 1 == end else [lent]
        out_turned = [turned(partner(layer + 1), weight, fresh) for weight in lenders]
        if layer < end - 1:
            state = jnp.where(c == layer, fresh, state)
        pieces = [moved(fresh, shifted(layer, layer + 1, k)) for k in send_order(ways)]

    mine, other = kept
    brought = moved(other, [(at(t1 // 2, end, t1), at(1 - t1 // 2, end, t1)) for t1 in range(ways)])
    residual = jnp.where(s == t // 2, mine, brought)
    outs = attend(aside, got_far, got_near, cosine, sine, out_turned, ways, block, features, heads)
    parts = []
    for k in send_order(ways):
        parts.append(moved(outs[k], shifted(partner(end), end, k)))
    third = moved(residual, shifted(end, partner(end), 0))
    return finish(parts, residual, third, earlier)


def passed_along(value, axis, steps):
    count = lax.axis_size(axis)
    leading, last = (max(0, -steps), min(count, count - steps))
    return lax.ppermute(value, axis, [(source, source + steps) for source in range(leading, last)])


def from_root(value, axis, root):
    mine = lax.axis_index(axis) == root
    return lax.psum(jnp.where(mine, value, jnp.zeros_like(value)), axis)


def rotate_half(heads, cosine_table, sine_values):
    half_width = heads.shape[-1] // 2
    first_half = heads[..., :half_width]
    second = heads[..., half_width:]
    cosine_table = cosine_table[:, None, :]
    sine_values = sine_values[:, None, :]
    return jnp.concatenate(
        [
            first_half * cosine_table - second * sine_values,
            second * cosine_table + first_half * sine_values,
        ],
        axis=-1,
    )


def norm_rows(row_block, gain_row):
    values = row_block.astype(jnp.float32)
    inverse_rms = lax.rsqrt(jnp.mean(values * values, axis=-1, keepdims=True) + EPS)
    return (values * inverse_rms * gain_row[None, :]).astype(jnp.bfloat16)


def gathered_project(full_rows, gain_row, qkv_full, positions, query_heads, key_value_heads):
    row_count = full_rows.shape[0]
    normed = norm_rows(full_rows, gain_row)
    projected_rows = jnp.dot(normed, qkv_full, preferred_element_type=jnp.float32)
    projected_rows = projected_rows.reshape(row_count, query_heads + 2 * key_value_heads, HEAD_WIDTH)
    cosine_table, sine_values = rope_tables(positions, HEAD_WIDTH)
    query_rows = rotate_half(projected_rows[:, :query_heads], cosine_table, sine_values)
    key_head_rows = rotate_half(
        projected_rows[:, query_heads : query_heads + key_value_heads], cosine_table, sine_values
    )
    value_head_rows = projected_rows[:, query_heads + key_value_heads :]
    return tuple(v.astype(jnp.bfloat16) for v in (query_rows, key_head_rows, value_head_rows))


def gathered_attend(query_rows, key_head_rows, value_head_rows, allowed):
    row_count, query_heads, head_size = query_rows.shape
    key_value_heads = key_head_rows.shape[1]
    query_groups = query_rows.reshape(row_count, key_value_heads, query_heads // key_value_heads, head_size)
    scores = jnp.einsum(
        "rkph,ckh->kprc", query_groups, key_head_rows, preferred_element_type=jnp.float32
    ) * head_size ** (-0.5)
    scores = jnp.where(allowed[None, None], scores, MASKED)
    weights = jax.nn.softmax(scores, axis=-1).astype(jnp.bfloat16)
    attended = jnp.einsum("kprc,ckh->rkph", weights, value_head_rows, preferred_element_type=jnp.float32)
    return attended.reshape(row_count, query_heads * head_size).astype(jnp.bfloat16)


def gathered_combine(current, attended, out_full):
    partial_value = lax.dot_general(
        attended, out_full, (((1,), (1,)), ((), ())), preferred_element_type=jnp.float32
    )
    summed = lax.psum_scatter(
        partial_value.astype(jnp.bfloat16), "tp", scatter_dimension=1, tiled=True
    ).astype(jnp.float32)
    return (current.astype(jnp.float32) + summed).astype(jnp.bfloat16)


def gathered_body(token_ids, embed_columns, norm_gain, qkv_weight, out_weight):
    seq_count = lax.axis_size("seq")
    section_count = lax.axis_size("section")
    tensor_parallel_count = lax.axis_size("tp")
    group_index = lax.axis_index("seq")
    section_index = lax.axis_index("section")
    block_row_slice = token_ids.shape[0]
    feature_cols = embed_columns.shape[0] * seq_count
    query_heads = QUERY_HEADS // tensor_parallel_count
    key_value_heads = KEY_VALUE_HEADS // tensor_parallel_count
    every_id = lax.all_gather(token_ids, "seq", axis=0, tiled=True)
    looked = jnp.take(embed_columns, every_id, axis=1)
    current = lax.all_to_all(looked, "seq", split_axis=1, concat_axis=0, tiled=True).T
    qkv_full = lax.all_gather(qkv_weight, "seq", axis=1, tiled=True)[0]
    out_full = lax.all_gather(out_weight, "seq", axis=1, tiled=True)[0]
    gain_row = norm_gain[0].astype(jnp.float32)
    outputs = jnp.zeros((block_row_slice, feature_cols), jnp.bfloat16)
    row_ids = jnp.arange(block_row_slice)[:, None]
    column = jnp.arange(2 * block_row_slice)[None, :]
    positions = group_index * block_row_slice + jnp.arange(block_row_slice)
    allowed = jnp.where(column < block_row_slice, group_index > 0, column - block_row_slice <= row_ids)
    for step_number in range(section_count):
        full_rows = lax.all_gather(current, "tp", axis=1, tiled=True)
        query_rows, key_head_rows, value_head_rows = gathered_project(
            full_rows, gain_row, qkv_full, positions, query_heads, key_value_heads
        )
        anchor_heads = from_root(key_head_rows, "seq", 0)
        anchor_values = from_root(value_head_rows, "seq", 0)
        both_keys = jnp.concatenate([anchor_heads, key_head_rows], axis=0)
        both_values = jnp.concatenate([anchor_values, value_head_rows], axis=0)
        attended = gathered_attend(query_rows, both_keys, both_values, allowed)
        new_rows = gathered_combine(current, attended, out_full)
        outputs = jnp.where(section_index == step_number, new_rows, outputs)
        if step_number + 1 < section_count:
            current = passed_along(new_rows, "section", 1)
    return outputs[None]


def solution(mesh):
    placed = (
        P("seq"),
        P(("tp", "seq"), None),
        P("section", None),
        P("section", "seq", "tp"),
        P("section", "seq", "tp"),
    )
    sizes = mesh.shape
    small = sizes["seq"] == 2 and sizes["tp"] == 4 and sizes["section"] == 4
    return jax.shard_map(
        stationary_body if small else gathered_body,
        mesh=mesh,
        in_specs=placed,
        out_specs=P("section", "seq", "tp"),
        check_vma=False,
    )
```

```python
import functools

import jax
import jax.numpy as jnp
import numpy as np
from jax import lax
from jax.experimental import pallas as pl
from jax.experimental.pallas import tpu as pltpu
from jax.sharding import PartitionSpec as P


QUERY_HEADS = 16
KEY_VALUE_HEADS = 8
HEAD_WIDTH = 128

EPS = 1e-05
ROPE_BASE = 500000.0
MASKED = -1e30
LANES = 128
AXES = ("seq", "section", "tp")


def rope_tables(positions, head_size):
    half_width = head_size // 2
    inverse_freq = ROPE_BASE ** (-jnp.arange(half_width).astype(jnp.float32) * (2.0 / head_size))
    angles = positions.astype(jnp.float32)[:, None] * inverse_freq[None, :]
    return (jnp.cos(angles), jnp.sin(angles))


def full_rope_tables(count, head_size):
    half_width = head_size // 2
    exponents = -np.arange(half_width).astype(np.float32) * np.float32(2.0 / head_size)
    inverse_freq = np.float32(ROPE_BASE) ** exponents
    angles = np.arange(count).astype(np.float32)[:, None] * inverse_freq[None, :]
    cosine, sine = np.cos(angles), np.sin(angles)
    return (
        np.concatenate([cosine, cosine], axis=1).astype(np.float32),
        np.concatenate([-sine, sine], axis=1).astype(np.float32),
    )


VMEM = pl.BlockSpec(memory_space=pltpu.VMEM)
SMEM = pl.BlockSpec(memory_space=pltpu.SMEM)
ANY = pl.BlockSpec(memory_space=pl.ANY)
HBM = pl.BlockSpec(memory_space=pltpu.HBM)


def on_section(kernel, section):
    def gated(*refs):
        pl.when(lax.axis_index("section") == section)(lambda: kernel(*refs))

    return gated


def lookup_kernel(ids_smem, ids_row, table, out, strips, onehot, sems):
    @pl.when(lax.axis_index("section") > 0)
    def _():
        read_columns(ids_smem, ids_row, table, out, strips, onehot, sems)


def read_columns(ids_smem, ids_row, table, out, strips, onehot, sems):
    features, _ = table.shape
    count = ids_row.shape[1]

    group = 8
    wide = group * LANES
    for i in range(count):
        first = pl.multiple_of((ids_smem[i] // LANES) * LANES, LANES)
        pltpu.make_async_copy(
            table.at[:, pl.ds(first, LANES)],
            strips.at[:, pl.ds(i * LANES, LANES)],
            sems.at[i // group],
        ).start()
    lanes = lax.rem(ids_row[...], LANES)
    acc = jnp.zeros((features, count), jnp.float32)
    rows = lax.broadcasted_iota(jnp.int32, (wide, count), 0)
    target = lax.broadcasted_iota(jnp.int32, (1, count), 1) * LANES + lanes
    for g in range(count // group):
        onehot[g] = jnp.where(rows == target - g * wide, 1.0, 0.0).astype(jnp.bfloat16)
    for g in range(count // group):
        there = pl.ds(g * wide, wide)
        pltpu.make_async_copy(table.at[:, pl.ds(0, wide)], strips.at[:, there], sems.at[g]).wait()
        acc = acc + jnp.dot(strips[:, there], onehot[g], preferred_element_type=jnp.float32)
    out[...] = acc.T.astype(jnp.bfloat16)


def lookup(ids, table):
    count, features = ids.shape[0], table.shape[0]
    return pl.pallas_call(
        lookup_kernel,
        out_shape=jax.ShapeDtypeStruct((count, features), jnp.bfloat16),
        in_specs=[SMEM, VMEM, ANY],
        out_specs=VMEM,
        scratch_shapes=[
            pltpu.VMEM((features, count * LANES), jnp.bfloat16),
            pltpu.VMEM((count // 8, 8 * LANES, count), jnp.bfloat16),
            pltpu.SemaphoreType.DMA((count // 8,)),
        ],
        name="lookup",
        compiler_params=pltpu.CompilerParams(vmem_limit_bytes=16 << 20),
    )(ids, ids.reshape(1, count), table)


def send_order(ways):
    return sorted(range(ways), key=lambda k: -min(k, ways - k))


def whole_piece(rank, k, ways, parts):
    if len(parts) == 1:
        return parts[0][...]
    even = lax.rem(rank + ways - k, 2) == 0
    first, second = parts[0][...], parts[1][...]
    return jnp.concatenate([jnp.where(even, first, second), jnp.where(even, second, first)], axis=0)


def project_kernel(*refs, ways, split, last):
    pieces, (gain, weight, message, *kept) = refs[: ways * split], refs[ways * split :]
    rank, group = lax.axis_index("tp"), lax.axis_index("seq")
    width = pieces[0].shape[1]
    squares = None
    acc = None
    for n, k in enumerate(send_order(ways)):
        piece = whole_piece(rank, k, ways, pieces[n * split : (n + 1) * split])
        if last:
            kept[2][:, pl.ds(pl.multiple_of(lax.rem(rank + ways - k, ways) * width, width), width)] = piece
        elif k == 0:
            kept[0][...] = piece
        values = piece.astype(jnp.float32)
        square = jnp.sum(values * values, axis=1, keepdims=True)
        squares = square if squares is None else squares + square
        first = pl.multiple_of(lax.rem(rank + ways - k, ways) * width, width)
        scaled = (values * gain[:, pl.ds(first, width)]).astype(jnp.bfloat16)
        part = jnp.dot(scaled, weight[0, pl.ds(first, width), :], preferred_element_type=jnp.float32)
        acc = part if acc is None else acc + part
    cols = acc.shape[1]
    message[:, :cols] = acc.astype(jnp.bfloat16)
    high = squares.astype(jnp.bfloat16)
    low = squares - high.astype(jnp.float32)
    lane = lax.broadcasted_iota(jnp.int32, (acc.shape[0], LANES), 1)
    message[:, cols:] = jnp.where(lane < LANES // 2, high.astype(jnp.float32), low).astype(jnp.bfloat16)
    if last:
        mine, other, whole = kept
        block, quarter = mine.shape
        first = pl.multiple_of(lax.rem(rank, 2) * quarter, quarter)
        mine[...] = whole[pl.ds(pl.multiple_of(group * block, block), block), pl.ds(first, quarter)]
        other[...] = whole[pl.ds(pl.multiple_of((1 - group) * block, block), block), pl.ds(first, quarter)]


def project(section, pieces, gain, weight, ways, last):
    split = len(pieces) // ways
    rows, width = pieces[0].shape[0] * split, pieces[0].shape[1]
    cols = weight.shape[2]
    kept = [(rows // 2, 2 * width)] * 2 if last else [(rows, width)]
    return pl.pallas_call(
        on_section(functools.partial(project_kernel, ways=ways, split=split, last=last), section),
        out_shape=[
            jax.ShapeDtypeStruct((rows, cols + LANES), jnp.bfloat16),
        ]
        + [jax.ShapeDtypeStruct(shape, jnp.bfloat16) for shape in kept],
        in_specs=[VMEM] * (len(pieces) + 2),
        out_specs=[VMEM] * (1 + len(kept)),
        scratch_shapes=[pltpu.VMEM((rows, ways * width), jnp.bfloat16)] if last else [],
        name="project",
        compiler_params=pltpu.CompilerParams(vmem_limit_bytes=6 << 20),
    )(*pieces, gain, weight)


def stage_kernel(weight, after, out, sem):
    copy = pltpu.make_async_copy(weight, out, sem)
    copy.start()
    copy.wait()


def stage(section, weight, after):
    return pl.pallas_call(
        on_section(stage_kernel, section),
        out_shape=jax.ShapeDtypeStruct(weight.shape, weight.dtype),
        in_specs=[HBM, ANY],
        out_specs=VMEM,
        scratch_shapes=[pltpu.SemaphoreType.DMA],
        name="stage",
        compiler_params=pltpu.CompilerParams(vmem_limit_bytes=1 << 20),
    )(weight, after)


def turn_kernel(weight, after, out, held, sem):
    copy = pltpu.make_async_copy(weight, held, sem)
    copy.start()
    copy.wait()
    out[...] = held[0].T


def turned(section, weight, after):
    return pl.pallas_call(
        on_section(turn_kernel, section),
        out_shape=jax.ShapeDtypeStruct(weight.shape[:0:-1], weight.dtype),
        in_specs=[HBM, ANY],
        out_specs=VMEM,
        scratch_shapes=[pltpu.VMEM(weight.shape, weight.dtype), pltpu.SemaphoreType.DMA],
        name="turn",
        compiler_params=pltpu.CompilerParams(vmem_limit_bytes=8 << 20),
    )(weight, after)


def attended_heads(total, inverse, cosine, sine, block, query_heads, key_value_heads, only):
    rows = total.shape[0]
    asked = rows if only is None else block
    repeat = query_heads // key_value_heads

    def head(i):
        return total[:, i * HEAD_WIDTH : (i + 1) * HEAD_WIDTH] * inverse

    def chosen(values):
        if only is None:
            return values
        blocks = [values[i * block : (i + 1) * block] for i in range(rows // block)]
        picked = blocks[0]
        for i in range(1, len(blocks)):
            picked = jnp.where(only == i, blocks[i], picked)
        return picked

    def rotated(i, pick=lambda values: values):
        values = pick(head(i))
        turned = values * pick(cosine) + pltpu.roll(values, HEAD_WIDTH // 2, 1) * pick(sine)
        return turned.astype(jnp.bfloat16)

    row = lax.broadcasted_iota(jnp.int32, (asked, rows), 0)
    row = row if only is None else row + only * block
    col = lax.broadcasted_iota(jnp.int32, (asked, rows), 1)
    row_block, col_block = row // block, col // block
    allowed = ((row_block == col_block) & (col <= row)) | ((col_block == 0) & (row_block > 0))
    keys = [rotated(query_heads + j) for j in range(key_value_heads)]
    held = [head(query_heads + key_value_heads + j).astype(jnp.bfloat16) for j in range(key_value_heads)]
    queries = [rotated(i, chosen) for i in range(query_heads)]
    scores = [times_transposed(query, keys[i // repeat]) * HEAD_WIDTH ** (-0.5) for i, query in enumerate(queries)]
    scores = [jnp.where(allowed, score, MASKED) for score in scores]
    tops = [jnp.max(score, axis=1, keepdims=True) for score in scores]
    powers = [jnp.exp(score - top) for score, top in zip(scores, tops)]
    sums = [jnp.sum(power, axis=1, keepdims=True) for power in powers]
    weights = [(power / total_power).astype(jnp.bfloat16) for power, total_power in zip(powers, sums)]
    results = [
        jnp.dot(weight, held[i // repeat], preferred_element_type=jnp.float32).astype(jnp.bfloat16)
        for i, weight in enumerate(weights)
    ]
    return jnp.concatenate(results, axis=1)


def summed(got, mine, features):
    cols = mine.shape[1] - LANES
    squares = sum(
        message[:, at : at + 1].astype(jnp.float32) for message in (got, mine) for at in (cols, cols + LANES // 2)
    )
    inverse = lax.rsqrt(squares / features + EPS)
    return mine[:, :cols].astype(jnp.float32) + got[:, :cols].astype(jnp.float32), inverse


def times_transposed(left, right):
    return lax.dot_general(left, right, (((1,), (1,)), ((), ())), preferred_element_type=jnp.float32)


def attend_kernel(got, mine, cosine, sine, weight, *outs, ways, block, features, heads):
    rank = lax.axis_index("tp")
    width = outs[0].shape[1]
    total, inverse = summed(got, mine, features)
    attended = attended_heads(total, inverse, cosine[...], sine[...], block, *heads, None)
    for k in range(ways):
        first = pl.multiple_of(lax.rem(rank + k, ways) * width, width)
        product = jnp.dot(attended, weight[:, pl.ds(first, width)], preferred_element_type=jnp.float32)
        outs[k][...] = product.astype(outs[k].dtype)


def last_kernel(got, mine, cosine, sine, weight, other_weight, *refs, ways, block, features, heads):
    outs, (slots,) = refs[:ways], refs[ways:]
    rank, group = lax.axis_index("tp"), lax.axis_index("seq")
    width = outs[0].shape[1]
    total, inverse = summed(got, mine, features)
    attended = attended_heads(total, inverse, cosine[...], sine[...], block, *heads, group)
    per_half = weight.shape[1] // width
    for side, held in ((group, weight), (1 - group, other_weight)):
        for i in range(per_half):
            shift = lax.rem(side * per_half + i + ways - rank, ways)
            columns = held[:, i * width : (i + 1) * width]
            slots[shift] = jnp.dot(attended, columns, preferred_element_type=jnp.float32).astype(slots.dtype)
    for k in range(ways):
        outs[k][...] = slots[k]


def attend(section, got, mine, cosine, sine, weights, ways, block, features, heads):
    last = len(weights) > 1
    shape = (block, features // ways) if last else (mine.shape[0], weights[0].shape[1] // ways)
    return pl.pallas_call(
        on_section(
            functools.partial(
                last_kernel if last else attend_kernel, ways=ways, block=block, features=features, heads=heads
            ),
            section,
        ),
        out_shape=[jax.ShapeDtypeStruct(shape, jnp.bfloat16) for _ in range(ways)],
        in_specs=[VMEM] * (4 + len(weights)),
        out_specs=[VMEM] * ways,
        scratch_shapes=[pltpu.VMEM((ways,) + shape, jnp.bfloat16)] if last else [],
        name="attend",
        compiler_params=pltpu.CompilerParams(vmem_limit_bytes=6 << 20),
    )(got, mine, cosine, sine, *weights)


def combine_kernel(*refs, ways):
    parts, (residual, out) = refs[:ways], refs[ways:]
    total = parts[0][...].astype(jnp.float32)
    for part in parts[1:]:
        total = total + part[...].astype(jnp.float32)
    out[...] = (residual[...].astype(jnp.float32) + total).astype(jnp.bfloat16)


def combine(parts, residual):
    return pl.pallas_call(
        functools.partial(combine_kernel, ways=len(parts)),
        out_shape=jax.ShapeDtypeStruct(residual.shape, jnp.bfloat16),
        in_specs=[VMEM] * (len(parts) + 1),
        out_specs=VMEM,
        name="combine",
        compiler_params=pltpu.CompilerParams(vmem_limit_bytes=4 << 20),
    )(*parts, residual)


def finish_kernel(*refs, ways):
    parts, (residual, third, first, second, out) = refs[:ways], refs[ways:]
    group, section = lax.axis_index("seq"), lax.axis_index("section")
    sections = lax.axis_size("section")
    width = first.shape[1]

    @pl.when(section == sections - 1)
    def _():
        total = parts[0][...].astype(jnp.float32)
        for part in parts[1:]:
            total = total + part[...].astype(jnp.float32)
        out[0] = (residual[...].astype(jnp.float32) + total).astype(jnp.bfloat16)

    @pl.when(section == sections - 2)
    def _():
        out[0] = third[...]

    @pl.when(section < sections - 2)
    def _():
        out[0, :, :width] = jnp.where(group == 0, first[...], second[...])
        out[0, :, width:] = jnp.where(group == 0, second[...], first[...])


def finish(parts, residual, third, earlier):
    return pl.pallas_call(
        functools.partial(finish_kernel, ways=len(parts)),
        out_shape=jax.ShapeDtypeStruct((1,) + residual.shape, jnp.bfloat16),
        in_specs=[VMEM] * (len(parts) + 4),
        out_specs=VMEM,
        name="finish",
        compiler_params=pltpu.CompilerParams(vmem_limit_bytes=4 << 20),
    )(*parts, residual, third, *earlier)


def stationary_body(token_ids, embed_columns, norm_gain, qkv_weight, out_weight):
    seq_count = lax.axis_size("seq")
    sections = lax.axis_size("section")
    ways = lax.axis_size("tp")
    s, c, t = lax.axis_index("seq"), lax.axis_index("section"), lax.axis_index("tp")
    block = token_ids.shape[0]
    rows = block * seq_count
    width = embed_columns.shape[0]
    half = qkv_weight.shape[1]
    features = half * seq_count
    heads = (QUERY_HEADS // ways, KEY_VALUE_HEADS // ways)

    def at(seq, section, tp):
        return (seq * sections + section) * ways + tp

    def moved(value, pairs):
        return lax.ppermute(value, AXES, pairs)

    gain = lax.dynamic_slice_in_dim(norm_gain, s * half, half, axis=1).astype(jnp.float32)
    cosine, sine = (jnp.asarray(table) for table in full_rope_tables(rows, HEAD_WIDTH))

    def partner(section):
        return section ^ 1

    everywhere = [(s1, t1) for s1 in range(seq_count) for t1 in range(ways)]

    lent = lax.ppermute(out_weight, "section", [(i, partner(i)) for i in range(sections)])
    end = sections - 1
    lent_far = moved(out_weight, [(at(s1, end, t1), at(1 - s1, partner(end), t1)) for s1, t1 in everywhere])

    other_ids = lax.ppermute(token_ids, "seq", [(0, 1), (1, 0)])
    servers = {0: lambda t1: 1, 1: lambda t1: 2 + t1 // 2}
    ids = jnp.where(c == 1, token_ids, other_ids)
    looked = lookup(ids, embed_columns)
    arrivals = {}
    for group in range(2):
        for k in send_order(ways):
            pairs = []
            for s1, t1 in everywhere:
                b = s1 * ways + (t1 - k) % ways
                pairs.append((at(b % seq_count, servers[group](t1), b // seq_count), at(s1, 0, t1)))
            arrivals[k, group] = moved(looked, pairs)
    staged = stage(0, qkv_weight, looked)
    out_turned = [turned(partner(0), lent, looked)]
    pieces = [arrivals[k, group] for k in send_order(ways) for group in range(2)]

    def shifted(source, target, k):
        if k == 0 and partner(source) == target:
            return [(at(s1, i, t1), at(s1, partner(i), t1)) for i in range(source % 2, sections, 2) for s1, t1 in everywhere]
        return [(at(s1, source, t1), at(s1, target, (t1 + k) % ways)) for s1, t1 in everywhere]

    def crossed(source):
        return [
            (at(s1, i, t1), at(1 - s1, partner(i), t1))
            for i in (range(0, sections, 2) if source % 2 == 0 else [source])
            for s1, t1 in everywhere
        ]

    state = jnp.zeros((rows, width), jnp.bfloat16)
    earlier = []
    for layer in range(sections):
        aside = partner(layer)
        message, *kept = project(layer, pieces, gain, staged, ways, layer == end)
        if layer == end - 1:
            state, _ = lax.optimization_barrier((state, message))
            for m in range(2):
                chosen = lax.dynamic_slice_in_dim(state, lax.rem(t + m, 2) * block, block, axis=0)
                pairs = []
                for section in range(end - 1):
                    for s2, t2 in everywhere:
                        pairs.append((at(s2, section, t2), at((t2 + m) % 2, section, 2 * s2 + t2 // 2)))
                earlier.append(moved(chosen, pairs))
        got_far = moved(message, crossed(layer))
        got_near = moved(message, shifted(layer, aside, 0))
        if layer == end:
            break
        outs = attend(aside, got_far, got_near, cosine, sine, out_turned, ways, block, features, heads)
        parts = [moved(outs[k], shifted(aside, layer, k)) for k in send_order(ways)]
        fresh = combine(parts, kept[0])
        staged = stage(layer + 1, qkv_weight, fresh)
        lenders = [lent, lent_far] if layer + 1 == end else [lent]
        out_turned = [turned(partner(layer + 1), weight, fresh) for weight in lenders]
        if layer < end - 1:
            state = jnp.where(c == layer, fresh, state)
        pieces = []
        for k in send_order(ways):
            pieces.append(moved(fresh, shifted(layer, layer + 1, k)))

    mine, other = kept
    brought = moved(other, [(at(t1 // 2, end, t1), at(1 - t1 // 2, end, t1)) for t1 in range(ways)])
    residual = jnp.where(s == t // 2, mine, brought)
    outs = attend(aside, got_far, got_near, cosine, sine, out_turned, ways, block, features, heads)
    parts = []
    for k in send_order(ways):
        parts.append(moved(outs[k], shifted(partner(end), end, k)))
    third = moved(residual, shifted(end, partner(end), 0))
    return finish(parts, residual, third, earlier)


def passed_along(value, axis, steps):
    count = lax.axis_size(axis)
    leading, last = (max(0, -steps), min(count, count - steps))
    return lax.ppermute(value, axis, [(source, source + steps) for source in range(leading, last)])


def from_root(value, axis, root):
    mine = lax.axis_index(axis) == root
    return lax.psum(jnp.where(mine, value, jnp.zeros_like(value)), axis)


def rotate_half(heads, cosine_table, sine_values):
    half_width = heads.shape[-1] // 2
    first_half = heads[..., :half_width]
    second = heads[..., half_width:]
    cosine_table = cosine_table[:, None, :]
    sine_values = sine_values[:, None, :]
    return jnp.concatenate(
        [
            first_half * cosine_table - second * sine_values,
            second * cosine_table + first_half * sine_values,
        ],
        axis=-1,
    )


def norm_rows(row_block, gain_row):
    values = row_block.astype(jnp.float32)
    inverse_rms = lax.rsqrt(jnp.mean(values * values, axis=-1, keepdims=True) + EPS)
    return (values * inverse_rms * gain_row[None, :]).astype(jnp.bfloat16)


def gathered_project(full_rows, gain_row, qkv_full, positions, query_heads, key_value_heads):
    row_count = full_rows.shape[0]
    normed = norm_rows(full_rows, gain_row)
    projected_rows = jnp.dot(normed, qkv_full, preferred_element_type=jnp.float32)
    projected_rows = projected_rows.reshape(row_count, query_heads + 2 * key_value_heads, HEAD_WIDTH)
    cosine_table, sine_values = rope_tables(positions, HEAD_WIDTH)
    query_rows = rotate_half(projected_rows[:, :query_heads], cosine_table, sine_values)
    key_head_rows = rotate_half(
        projected_rows[:, query_heads : query_heads + key_value_heads], cosine_table, sine_values
    )
    value_head_rows = projected_rows[:, query_heads + key_value_heads :]
    return tuple(v.astype(jnp.bfloat16) for v in (query_rows, key_head_rows, value_head_rows))


def gathered_attend(query_rows, key_head_rows, value_head_rows, allowed):
    row_count, query_heads, head_size = query_rows.shape
    key_value_heads = key_head_rows.shape[1]
    query_groups = query_rows.reshape(row_count, key_value_heads, query_heads // key_value_heads, head_size)
    scores = jnp.einsum(
        "rkph,ckh->kprc", query_groups, key_head_rows, preferred_element_type=jnp.float32
    ) * head_size ** (-0.5)
    scores = jnp.where(allowed[None, None], scores, MASKED)
    weights = jax.nn.softmax(scores, axis=-1).astype(jnp.bfloat16)
    attended = jnp.einsum("kprc,ckh->rkph", weights, value_head_rows, preferred_element_type=jnp.float32)
    return attended.reshape(row_count, query_heads * head_size).astype(jnp.bfloat16)


def gathered_combine(current, attended, out_full):
    partial_value = lax.dot_general(
        attended, out_full, (((1,), (1,)), ((), ())), preferred_element_type=jnp.float32
    )
    summed = lax.psum_scatter(
        partial_value.astype(jnp.bfloat16), "tp", scatter_dimension=1, tiled=True
    ).astype(jnp.float32)
    return (current.astype(jnp.float32) + summed).astype(jnp.bfloat16)


def gathered_body(token_ids, embed_columns, norm_gain, qkv_weight, out_weight):
    seq_count = lax.axis_size("seq")
    section_count = lax.axis_size("section")
    tensor_parallel_count = lax.axis_size("tp")
    group_index = lax.axis_index("seq")
    section_index = lax.axis_index("section")
    block_row_slice = token_ids.shape[0]
    feature_cols = embed_columns.shape[0] * seq_count
    query_heads = QUERY_HEADS // tensor_parallel_count
    key_value_heads = KEY_VALUE_HEADS // tensor_parallel_count
    every_id = lax.all_gather(token_ids, "seq", axis=0, tiled=True)
    looked = jnp.take(embed_columns, every_id, axis=1)
    current = lax.all_to_all(looked, "seq", split_axis=1, concat_axis=0, tiled=True).T
    qkv_full = lax.all_gather(qkv_weight, "seq", axis=1, tiled=True)[0]
    out_full = lax.all_gather(out_weight, "seq", axis=1, tiled=True)[0]
    gain_row = norm_gain[0].astype(jnp.float32)
    outputs = jnp.zeros((block_row_slice, feature_cols), jnp.bfloat16)
    row_ids = jnp.arange(block_row_slice)[:, None]
    column = jnp.arange(2 * block_row_slice)[None, :]
    positions = group_index * block_row_slice + jnp.arange(block_row_slice)
    allowed = jnp.where(column < block_row_slice, group_index > 0, column - block_row_slice <= row_ids)
    for step_number in range(section_count):
        full_rows = lax.all_gather(current, "tp", axis=1, tiled=True)
        query_rows, key_head_rows, value_head_rows = gathered_project(
            full_rows, gain_row, qkv_full, positions, query_heads, key_value_heads
        )
        anchor_heads = from_root(key_head_rows, "seq", 0)
        anchor_values = from_root(value_head_rows, "seq", 0)
        both_keys = jnp.concatenate([anchor_heads, key_head_rows], axis=0)
        both_values = jnp.concatenate([anchor_values, value_head_rows], axis=0)
        attended = gathered_attend(query_rows, both_keys, both_values, allowed)
        new_rows = gathered_combine(current, attended, out_full)
        outputs = jnp.where(section_index == step_number, new_rows, outputs)
        if step_number + 1 < section_count:
            current = passed_along(new_rows, "section", 1)
    return outputs[None]


def solution(mesh):
    placed = (
        P("seq"),
        P(("tp", "seq"), None),
        P("section", None),
        P("section", "seq", "tp"),
        P("section", "seq", "tp"),
    )
    sizes = mesh.shape
    small = sizes["seq"] == 2 and sizes["tp"] == 4 and sizes["section"] == 4
    return jax.shard_map(
        stationary_body if small else gathered_body,
        mesh=mesh,
        in_specs=placed,
        out_specs=P("section", "seq", "tp"),
        check_vma=False,
    )
```
